128 devices in a mesh: dp: 1, sp: 128 (over z, y, x, core).
Axes of the slice: x: 4, y: 4, z: 4, core: 2. Of those that a mesh axis runs over, the one named last changes fastest.
Arguments:
- x_in: bfloat16 [65536, 512], P(('dp', 'sp'))
- w_q: bfloat16 [512, 512], replicated
- w_k: bfloat16 [512, 512], replicated
- w_v: bfloat16 [512, 512], replicated
- w_o: bfloat16 [512, 512], replicated
- dy_in: bfloat16 [65536, 512], P(('dp', 'sp'))
Outputs:
- output 1: bfloat16 [65536, 512], P(('dp', 'sp'))
- output 2: bfloat16 [65536, 512], P(('dp', 'sp'))
- output 3: float32 [512, 512], P('dp')
- output 4: float32 [512, 512], P('dp')
- output 5: float32 [512, 512], P('dp')
- output 6: float32 [512, 512], P('dp')
All inputs are finite; a program needn't handle non-finite values.
Results may differ from the reference program's by a relative error of at most 0.0120032.
Values are sent between devices in bfloat16 or wider.
A program may use at most 1 GiB of HBM per device.

```python
import jax
import jax.numpy as jnp
from jax import lax

D = 512
HEADS = 8
HEAD = 64
TOKENS_DEV = 512
SP = 128
TOKENS = SP * TOKENS_DEV
DILATIONS = (1, 2, 4, 8)


def setup_inputs(seed: int = 0, part: int = 0) -> dict:
    root_key = jax.random.key(seed)
    sub_keys = jax.random.split(root_key, 6)
    x_key = jax.random.fold_in(sub_keys[0], part)
    dy_key = jax.random.fold_in(sub_keys[1], part)
    in_scale = D ** -0.5
    out_scale = (TOKENS_DEV / (4.0 * D)) ** 0.5
    x_in = jax.random.normal(x_key, (TOKENS, D), jnp.float32)
    dy_in = jax.random.normal(dy_key, (TOKENS, D), jnp.float32)
    w_q = jax.random.normal(sub_keys[2], (D, D), jnp.float32) * in_scale
    w_k = jax.random.normal(sub_keys[3], (D, D), jnp.float32) * in_scale
    w_v = jax.random.normal(sub_keys[4], (D, D), jnp.float32) * in_scale
    w_o = jax.random.normal(sub_keys[5], (D, D), jnp.float32) * out_scale
    return {'x_in': x_in.astype(jnp.bfloat16), 'w_q': w_q.astype(jnp.bfloat16), 'w_k': w_k.astype(jnp.bfloat16), 'w_v': w_v.astype(jnp.bfloat16), 'w_o': w_o.astype(jnp.bfloat16), 'dy_in': dy_in.astype(jnp.bfloat16)}


def project(left_rows, weight):
    return jnp.dot(left_rows, weight, preferred_element_type=jnp.float32).astype(jnp.bfloat16)


def pick_rows(values, dilation, seg_len):
    split_view = values.reshape(TOKENS // seg_len, seg_len // dilation, dilation, HEADS // dilation, dilation, HEAD)
    return jnp.stack([split_view[:, :, residue, :, residue, :] for residue in range(dilation)], axis=3)


def segment_attention(blocks):
    q_seg, k_seg, v_seg = blocks
    logits = jnp.einsum('iacd,jacd->acij', q_seg, k_seg)
    row_max = lax.stop_gradient(jnp.max(logits, axis=-1, keepdims=True))
    exp_logits = jnp.exp(logits - row_max)
    row_sum = jnp.sum(exp_logits, axis=-1, keepdims=True)
    seg_out = jnp.einsum('acij,jacd->iacd', exp_logits / row_sum, v_seg)
    seg_lse = jnp.transpose((row_max + jnp.log(row_sum))[..., 0], (2, 0, 1))
    return seg_out, seg_lse


def attention_core(q_f, k_f, v_f):
    q_scaled = q_f * HEAD ** -0.5
    branch_outs = []
    branch_lses = []
    for dilation in DILATIONS:
        seg_len = TOKENS_DEV * dilation // 2
        picked = (pick_rows(q_scaled, dilation, seg_len), pick_rows(k_f, dilation, seg_len), pick_rows(v_f, dilation, seg_len))
        seg_out, seg_lse = lax.map(jax.checkpoint(segment_attention), picked)
        eye_f = jnp.eye(dilation, dtype=q_f.dtype)
        eye_b = jnp.eye(dilation, dtype=bool)
        spread = seg_out[:, :, None] * eye_f[None, None, :, None, :, None]
        branch_outs.append(spread.reshape(TOKENS, HEADS, HEAD))
        lse_spread = jnp.where(eye_b[None, None, :, None, :], seg_lse[:, :, None], -jnp.inf)
        branch_lses.append(lse_spread.reshape(TOKENS, HEADS))
    lse_stack = jnp.stack(branch_lses)
    lse_max = lax.stop_gradient(jnp.max(lse_stack, axis=0))
    branch_w = jnp.exp(lse_stack - lse_max)
    merged = jnp.sum(branch_w[..., None] * jnp.stack(branch_outs), axis=0) / jnp.sum(branch_w, axis=0)[..., None]
    return merged.reshape(TOKENS, D)


def reference(x_in, w_q, w_k, w_v, w_o, dy_in):
    q_rows = project(x_in, w_q)
    k_rows = project(x_in, w_k)
    v_rows = project(x_in, w_v)
    attn_out, core_vjp = jax.vjp(attention_core, q_rows.astype(jnp.float32), k_rows.astype(jnp.float32), v_rows.astype(jnp.float32))
    attn_b = attn_out.astype(jnp.bfloat16)
    y_out = project(attn_b, w_o)
    d_attn = project(dy_in, w_o.T)
    grad_q, grad_k, grad_v = core_vjp(d_attn.astype(jnp.float32))
    dq_b = grad_q.astype(jnp.bfloat16)
    dk_b = grad_k.astype(jnp.bfloat16)
    dv_b = grad_v.astype(jnp.bfloat16)
    dx_sum = jnp.dot(dq_b, w_q.T, preferred_element_type=jnp.float32) + jnp.dot(dk_b, w_k.T, preferred_element_type=jnp.float32) + jnp.dot(dv_b, w_v.T, preferred_element_type=jnp.float32)
    dx_out = dx_sum.astype(jnp.bfloat16)
    dw_q = jnp.dot(x_in.T, dq_b, preferred_element_type=jnp.float32)
    dw_k = jnp.dot(x_in.T, dk_b, preferred_element_type=jnp.float32)
    dw_v = jnp.dot(x_in.T, dv_b, preferred_element_type=jnp.float32)
    dw_o = jnp.dot(attn_b.T, dy_in, preferred_element_type=jnp.float32)
    return y_out, dx_out, dw_q, dw_k, dw_v, dw_o
```

```python
import functools

import jax
import jax.numpy as jnp
from jax import lax
from jax.experimental import pallas as pl
from jax.experimental.pallas import tpu as pltpu
from jax.sharding import PartitionSpec as P

HEAD_DIM = 64
F32 = jnp.float32
BF16 = jnp.bfloat16
MESH = pl.DeviceIdType.MESH
NN = (((1,), (0,)), ((), ()))
NT = (((1,), (1,)), ((), ()))
TN = (((0,), (0,)), ((), ()))


def dot(a, b, dims=NN):
    return lax.dot_general(a, b, dims, preferred_element_type=F32)


def two(ref, lead, start, n):
    return jnp.concatenate([ref[lead + (pl.ds(start, n), slice(None))], ref[lead + (pl.ds(256 + start, n), slice(None))]], axis=0)


def put_two(ref, lead, start, n, val):
    ref[lead + (pl.ds(start, n), slice(None))] = val[:n]
    ref[lead + (pl.ds(256 + start, n), slice(None))] = val[n:]


def wide(stat):
    return jnp.concatenate([stat, stat], axis=1)


def lanes_low(rows):
    return lax.broadcasted_iota(jnp.int32, (rows, 128), 1) < 64


def attention_kernel(x_ref, wq_ref, wk_ref, wv_ref, wo_ref, dy_ref, y_ref, dx_ref, dw_ref,
                     xp, dyp, qm, kt, vt, dom, g2, g3, est, ms, mh, lh, oh, lseh, delh, dqh, dka, dva, attnb, grads,
                     st2, st3, colt, rowt, s2s, s2r, s3s, s3r, t2s, t2r, t3s, t3r):
    me = lax.axis_index("sp")
    member = me % 4
    base = me - member
    peers = [None, base + (member + 1 - 2 * (member % 2)), base + (member + 2 - 4 * (member // 2)), base + 3 - member]

    barrier = pltpu.get_barrier_semaphore()
    for p in peers[1:]:
        pl.semaphore_signal(barrier, inc=1, device_id={"sp": p}, device_id_type=MESH)

    ri = lax.broadcasted_iota(jnp.int32, (256, 256), 0)
    ci = lax.broadcasted_iota(jnp.int32, (256, 256), 1)

    def token_of(i):
        blk = i >> 5
        return ((i & 31) << 3) + ((blk & 1) << 2) + (blk & 2) + (blk >> 2)

    one = jnp.ones((), F32)
    zero = jnp.zeros((), F32)
    perm = jnp.where(token_of(ri) == ci, one, zero).astype(BF16)
    for s in range(2):
        rows = slice(256 * s, 256 * s + 256)
        xp[rows, :] = dot(perm, x_ref[rows, :]).astype(BF16)
        dyp[rows, :] = dot(perm, dy_ref[rows, :]).astype(BF16)

    low = lanes_low(512)
    keep = [jnp.where(low, one, zero).astype(BF16), jnp.where(low, zero, one).astype(BF16)]

    for half in range(2):
        cols = slice(256 * half, 256 * half + 256)
        qq = dot(xp[...], wq_ref[:, cols]).astype(BF16) * jnp.asarray(HEAD_DIM ** -0.5, BF16)
        kk = dot(xp[...], wk_ref[:, cols]).astype(BF16)
        vv = dot(xp[...], wv_ref[:, cols]).astype(BF16)
        dd = dot(dyp[...], wo_ref[cols, :], NT).astype(BF16)
        for u in range(2):
            t = 2 * half + u
            lanes = slice(128 * u, 128 * u + 128)
            kt[t] = kk[:, lanes]
            vt[t] = vv[:, lanes]
            for par in range(2):
                qm[par, t] = qq[:, lanes] * keep[par]
                dom[par, t] = dd[:, lanes] * keep[par]
            for g, n, off in ((g2, 64, 64 * (t & 1)), (g3, 32, 32 * (2 * (t & 1) + (t >> 1)))):
                for a, ref in ((0, kk), (1, vv)):
                    for s in range(2):
                        r = 256 * s + off
                        g[a, t, n * s:n * s + n, :] = ref[r:r + n, lanes] * keep[0][:n] + ref[r + 128:r + 128 + n, lanes] * keep[1][:n]
                for a, ref in ((2, qq), (3, dd)):
                    for s in range(2):
                        r = 256 * s + off
                        g[a, t, n * s:n * s + n, :] = ref[r:r + n, lanes] * keep[0][:n] + ref[r + 128:r + 128 + n, lanes] * keep[1][:n]

    pl.semaphore_wait(barrier, 3)
    copies2 = []
    copies3 = []
    for a in range(4):
        c = pltpu.make_async_remote_copy(src_ref=g2.at[a, :, pl.ds(0, 128), :], dst_ref=g2.at[a, :, pl.ds(128, 128), :],
                                         send_sem=s2s.at[a], recv_sem=s2r.at[a], device_id={"sp": peers[1]}, device_id_type=MESH)
        c.start()
        copies2.append(c)
    for a in range(4):
        row = []
        for d in (2, 3, 1):
            c = pltpu.make_async_remote_copy(src_ref=g3.at[a, :, pl.ds(0, 64), :], dst_ref=g3.at[a, :, pl.ds(64 * d, 64), :],
                                             send_sem=s3s.at[a, d], recv_sem=s3r.at[a, d], device_id={"sp": peers[d]}, device_id_type=MESH)
            c.start()
            row.append(c)
        copies3.append(row)

    def forward(q, k, v):
        s = dot(q, k, NT)
        m = jnp.max(s, axis=1, keepdims=True)
        e = jnp.exp(s - m)
        l = jnp.sum(e, axis=1, keepdims=True)
        o = dot(e.astype(BF16), v)
        n = q.shape[0]
        return jnp.broadcast_to(m, (n, 128)), jnp.broadcast_to(l, (n, 128)), o, e

    def merge(t, par, start, n, m, l, o):
        m0 = two(mh, (t, par), start, n)
        l0 = two(lh, (t, par), start, n)
        o0 = two(oh, (t, par), start, n)
        mn = jnp.maximum(m0, m)
        a = jnp.exp(m0 - mn)
        b = jnp.exp(m - mn)
        put_two(mh, (t, par), start, n, mn)
        put_two(lh, (t, par), start, n, l0 * a + l * b)
        put_two(oh, (t, par), start, n, o0 * a + o * b)

    def off2(t, par):
        return pl.multiple_of(128 * par + 64 * (t % 2), 64)

    def off3(t, par):
        return pl.multiple_of(128 * par + 64 * (t % 2) + 32 * (t // 2), 32)

    def fwd_local(t, carry):
        for par in range(2):
            for s in range(2):
                rows = slice(256 * s, 256 * s + 256)
                m, l, o, e = forward(qm[par, t, rows, :], kt[t, rows, :], vt[t, rows, :])
                mh[t, par, rows, :] = m
                lh[t, par, rows, :] = l
                oh[t, par, rows, :] = o
                ms[t, par, rows, :] = m
                est[t, par, rows, :] = e
            m, l, o, e = forward(two(qm, (par, t), 128 * par, 128), two(kt, (t,), 128 * par, 128), two(vt, (t,), 128 * par, 128))
            ms[t, par, 512:768, :] = m
            est[t, par, 512:768, :] = e
            merge(t, par, 128 * par, 128, m, l, o)
        return carry

    lax.fori_loop(0, 4, fwd_local, 0)

    for a in range(2):
        copies2[a].wait_recv()
        for c in copies3[a]:
            c.wait_recv()

    low256 = lanes_low(256)
    colt[...] = jnp.zeros_like(colt)

    def fwd_group(t, carry):
        atts = []
        for par in range(2):
            o2 = off2(t, par)
            m, l, o, e = forward(two(qm, (par, t), o2, 64), g2[0, t], g2[1, t])
            ms[t, par, 768:896, :] = m
            est[t, par, 768:896, :] = e
            merge(t, par, o2, 64, m, l, o)
            o3 = off3(t, par)
            m, l, o, e = forward(two(qm, (par, t), o3, 32), g3[0, t], g3[1, t])
            ms[t, par, 896:960, :] = m
            est[t, par, 896:960, :] = e
            merge(t, par, o3, 32, m, l, o)
            lt = lh[t, par]
            att = oh[t, par] / lt
            lse = mh[t, par] + jnp.log(lt)
            delta = jnp.broadcast_to(jnp.sum(dom[par, t].astype(F32) * att, axis=1, keepdims=True), (512, 128))
            lseh[t, par] = lse
            delh[t, par] = delta
            atts.append(att)
            h = 2 * t + par
            lane = lax.broadcasted_iota(jnp.int32, (512, 128), 1)
            colt[0:512, :] = jnp.where(lane == h, lse, jnp.where(lane == h + 8, delta, colt[0:512, :]))
            l2 = two(lseh, (t, par), o2, 64)
            d2 = two(delh, (t, par), o2, 64)
            colt[512:640, :] = jnp.where(lane[:128] == h, l2, jnp.where(lane[:128] == h + 8, d2, colt[512:640, :]))
            l3 = two(lseh, (t, par), o3, 32)
            d3 = two(delh, (t, par), o3, 32)
            l3 = jnp.concatenate([l3, l3], axis=0)
            d3 = jnp.concatenate([d3, d3], axis=0)
            colt[640:768, :] = jnp.where(lane[:128] == h, l3, jnp.where(lane[:128] == h + 8, d3, colt[640:768, :]))
        attnb[:, pl.ds(pl.multiple_of(128 * t, 128), 128)] = jnp.where(low, atts[0], atts[1]).astype(BF16)
        return carry

    lax.fori_loop(0, 4, fwd_group, 0)

    st2[0] = jnp.transpose(colt[512:640, :])[:16]
    st3[0] = jnp.transpose(colt[640:768, :])[:16]
    for j in range(4):
        r = jnp.transpose(colt[128 * j:128 * j + 128, :])
        rowt[:, 128 * j:128 * j + 128] = r[:16]
    stat2 = pltpu.make_async_remote_copy(src_ref=st2.at[0], dst_ref=st2.at[1], send_sem=t2s, recv_sem=t2r,
                                         device_id={"sp": peers[1]}, device_id_type=MESH)
    stat2.start()
    stats3 = []
    for d in (2, 3, 1):
        c = pltpu.make_async_remote_copy(src_ref=st3.at[0], dst_ref=st3.at[d], send_sem=t3s.at[d], recv_sem=t3r.at[d],
                                         device_id={"sp": peers[d]}, device_id_type=MESH)
        c.start()
        stats3.append(c)

    yb = dot(attnb[...], wo_ref[...]).astype(BF16)
    for s in range(2):
        rows = slice(256 * s, 256 * s + 256)
        y_ref[rows, :] = dot(perm, yb[rows, :], TN).astype(BF16)
    dw_ref[3] = dot(attnb[...], dyp[...], TN)

    def grad_q(d_rows, k, v, e, delta):
        dp = dot(d_rows, v, NT)
        ds = (e * (dp - wide(delta))).astype(BF16)
        return dot(ds, k)

    def grad_kv(q, d_rows, k, v, lse_row, delta_row):
        st = dot(k, q, NT)
        pt = jnp.exp(st - lse_row)
        dpt = dot(v, d_rows, NT)
        dst = (pt * (dpt - delta_row)).astype(BF16)
        return dot(dst, q), dot(pt.astype(BF16), d_rows)

    def row_of(ref, lead, i):
        return ref[lead + (pl.ds(i, 1), slice(None))]

    def bwd_local(t, carry):
        for par in range(2):
            h = 2 * t + par
            lse_row = row_of(rowt, (), h)
            del_row = row_of(rowt, (), h + 8)
            for s in range(2):
                rows = slice(256 * s, 256 * s + 256)
                dr = dom[par, t, rows, :]
                kr = kt[t, rows, :]
                vr = vt[t, rows, :]
                lse = lseh[t, par, rows, :]
                dqj = grad_q(dr, kr, vr, est[t, par, rows, :], delh[t, par, rows, :])
                dqh[par, rows, :] = dqj * jnp.exp(ms[t, par, rows, :] - lse)
                gk, gv = grad_kv(qm[par, t, rows, :], dr, kr, vr, lse_row[:, rows], del_row[:, rows])
                if par == 0:
                    dka[t, rows, :] = gk
                    dva[t, rows, :] = gv
                else:
                    dka[t, rows, :] += gk
                    dva[t, rows, :] += gv
            a = 128 * par
            dr = two(dom, (par, t), a, 128)
            kr = two(kt, (t,), a, 128)
            vr = two(vt, (t,), a, 128)
            f = jnp.exp(ms[t, par, 512:768, :] - two(lseh, (t, par), a, 128))
            dqj = f * grad_q(dr, kr, vr, est[t, par, 512:768, :], two(delh, (t, par), a, 128))
            put_two(dqh, (par,), a, 128, two(dqh, (par,), a, 128) + dqj)
            lr = jnp.concatenate([lse_row[:, a:a + 128], lse_row[:, 256 + a:256 + a + 128]], axis=1)
            dlr = jnp.concatenate([del_row[:, a:a + 128], del_row[:, 256 + a:256 + a + 128]], axis=1)
            gk, gv = grad_kv(two(qm, (par, t), a, 128), dr, kr, vr, lr, dlr)
            put_two(dka, (t,), a, 128, two(dka, (t,), a, 128) + gk)
            put_two(dva, (t,), a, 128, two(dva, (t,), a, 128) + gv)
            for lo, n, off, g in ((768, 64, off2(t, par), g2), (896, 32, off3(t, par), g3)):
                f = jnp.exp(ms[t, par, lo:lo + 2 * n, :] - two(lseh, (t, par), off, n))
                dqj = f * grad_q(two(dom, (par, t), off, n), g[0, t], g[1, t], est[t, par, lo:lo + 2 * n, :], two(delh, (t, par), off, n))
                put_two(dqh, (par,), off, n, two(dqh, (par,), off, n) + dqj)
        dq = jnp.where(low, dqh[0], dqh[1]) * (HEAD_DIM ** -0.5)
        grads[0, :, pl.ds(pl.multiple_of(128 * t, 128), 128)] = dq.astype(BF16)
        return carry

    lax.fori_loop(0, 4, bwd_local, 0)

    stat2.wait_recv()
    for c in stats3:
        c.wait_recv()
    for a in (2, 3):
        copies2[a].wait_recv()
        for c in copies3[a]:
            c.wait_recv()

    keep256 = [keep[0][:256], keep[1][:256]]

    def bwd_group(t, carry):
        for par in range(2):
            h = 2 * t + par
            lr = jnp.concatenate([row_of(st2, (0,), h), row_of(st2, (1,), h)], axis=1)
            dlr = jnp.concatenate([row_of(st2, (0,), h + 8), row_of(st2, (1,), h + 8)], axis=1)
            off = off2(t, par)
            gk, gv = grad_kv(g2[2, t] * keep256[par], g2[3, t] * keep256[par], two(kt, (t,), off, 64), two(vt, (t,), off, 64), lr, dlr)
            put_two(dka, (t,), off, 64, two(dka, (t,), off, 64) + gk)
            put_two(dva, (t,), off, 64, two(dva, (t,), off, 64) + gv)
            lo = lax.broadcasted_iota(jnp.int32, (1, 128), 1) < 64
            lr = jnp.concatenate([jnp.where(lo, row_of(st3, (0,), h), row_of(st3, (1,), h)), jnp.where(lo, row_of(st3, (2,), h), row_of(st3, (3,), h))], axis=1)
            dlr = jnp.concatenate([jnp.where(lo, row_of(st3, (0,), h + 8), row_of(st3, (1,), h + 8)), jnp.where(lo, row_of(st3, (2,), h + 8), row_of(st3, (3,), h + 8))], axis=1)
            off = off3(t, par)
            gk, gv = grad_kv(g3[2, t] * keep256[par], g3[3, t] * keep256[par], two(kt, (t,), off, 32), two(vt, (t,), off, 32), lr, dlr)
            put_two(dka, (t,), off, 32, two(dka, (t,), off, 32) + gk)
            put_two(dva, (t,), off, 32, two(dva, (t,), off, 32) + gv)
        cols = pl.ds(pl.multiple_of(128 * t, 128), 128)
        grads[1, :, cols] = dka[t].astype(BF16)
        grads[2, :, cols] = dva[t].astype(BF16)
        return carry

    lax.fori_loop(0, 4, bwd_group, 0)

    dxb = (dot(grads[0], wq_ref[...], NT) + dot(grads[1], wk_ref[...], NT) + dot(grads[2], wv_ref[...], NT)).astype(BF16)
    for s in range(2):
        rows = slice(256 * s, 256 * s + 256)
        dx_ref[rows, :] = dot(perm, dxb[rows, :], TN).astype(BF16)
    for i in range(3):
        dw_ref[i] = dot(xp[...], grads[i], TN)

    for c in copies2:
        c.wait_send()
    for row in copies3:
        for c in row:
            c.wait_send()
    stat2.wait_send()
    for c in stats3:
        c.wait_send()


def attention(x_loc, w_q, w_k, w_v, w_o, dy_loc):
    vmem = pl.BlockSpec(memory_space=pltpu.VMEM)
    sem = pltpu.SemaphoreType.DMA
    return pl.pallas_call(
        attention_kernel,
        out_shape=[jax.ShapeDtypeStruct((512, 512), BF16), jax.ShapeDtypeStruct((512, 512), BF16), jax.ShapeDtypeStruct((4, 512, 512), F32)],
        in_specs=[vmem] * 6,
        out_specs=[vmem] * 3,
        scratch_shapes=[
            pltpu.VMEM((512, 512), BF16), pltpu.VMEM((512, 512), BF16),
            pltpu.VMEM((2, 4, 512, 128), BF16), pltpu.VMEM((4, 512, 128), BF16), pltpu.VMEM((4, 512, 128), BF16), pltpu.VMEM((2, 4, 512, 128), BF16),
            pltpu.VMEM((4, 4, 256, 128), BF16), pltpu.VMEM((4, 4, 256, 128), BF16),
            pltpu.VMEM((4, 2, 960, 256), F32), pltpu.VMEM((4, 2, 960, 128), F32),
            pltpu.VMEM((4, 2, 512, 128), F32), pltpu.VMEM((4, 2, 512, 128), F32), pltpu.VMEM((4, 2, 512, 128), F32),
            pltpu.VMEM((4, 2, 512, 128), F32), pltpu.VMEM((4, 2, 512, 128), F32),
            pltpu.VMEM((2, 512, 128), F32), pltpu.VMEM((4, 512, 128), F32), pltpu.VMEM((4, 512, 128), F32),
            pltpu.VMEM((512, 512), BF16), pltpu.VMEM((3, 512, 512), BF16),
            pltpu.VMEM((2, 16, 128), F32), pltpu.VMEM((4, 16, 128), F32), pltpu.VMEM((768, 128), F32), pltpu.VMEM((16, 512), F32),
            sem((4,)), sem((4,)), sem((4, 4)), sem((4, 4)), sem, sem, sem((4,)), sem((4,)),
        ],
        compiler_params=pltpu.CompilerParams(collective_id=0, has_side_effects=True, vmem_limit_bytes=60 * 2 ** 20),
        name="attention_step",
    )(x_loc, w_q, w_k, w_v, w_o, dy_loc)


def solution(mesh):
    def device_step(x_loc, w_q, w_k, w_v, w_o, dy_loc):
        y_loc, dx_loc, dws = attention(x_loc, w_q, w_k, w_v, w_o, dy_loc)
        dws = lax.psum(dws, "sp")
        return y_loc, dx_loc, dws[0], dws[1], dws[2], dws[3]

    row_spec = P(("dp", "sp"), None)
    full_spec = P(None, None)
    grad_spec = P("dp", None)
    return jax.shard_map(device_step, mesh=mesh, in_specs=(row_spec, full_spec, full_spec, full_spec, full_spec, row_spec),
                         out_specs=(row_spec, row_spec, grad_spec, grad_spec, grad_spec, grad_spec), check_vma=False)
```

```python
import functools

import jax
import jax.numpy as jnp
from jax import lax
from jax.experimental import pallas as pl
from jax.experimental.pallas import tpu as pltpu
from jax.sharding import PartitionSpec as P

HEAD_DIM = 64
N4 = 4
N8 = 8
N16 = 16
N32 = 32
N64 = 64
N128 = 128
N256 = 256
N512 = 512
N640 = 640
N768 = 768
N896 = 896
N1024 = 1024
F32 = jnp.float32
BF16 = jnp.bfloat16
MESH = pl.DeviceIdType.MESH
NN = (((1,), (0,)), ((), ()))
NT = (((1,), (1,)), ((), ()))
TN = (((0,), (0,)), ((), ()))


def dot(a, b, dims=NN):
    return lax.dot_general(a, b, dims, preferred_element_type=F32)


def two(ref, lead, start, n):
    return jnp.concatenate([ref[lead + (pl.ds(start, n), slice(None))], ref[lead + (pl.ds(N256 + start, n), slice(None))]], axis=0)


def put_two(ref, lead, start, n, val):
    ref[lead + (pl.ds(start, n), slice(None))] = val[:n]
    ref[lead + (pl.ds(N256 + start, n), slice(None))] = val[n:]


def wide(stat):
    return jnp.concatenate([stat, stat], axis=1)


def lanes_low(rows):
    return lax.broadcasted_iota(jnp.int32, (rows, N128), 1) < N64


def attention_kernel(x_ref, wq_ref, wk_ref, wv_ref, wo_ref, dy_ref, y_ref, dx_ref, dw_ref,
                     xp, dyp, qm, kt, vt, dom, g2, g3, est, ms, mh, lh, oh, lseh, delh, dqh, dka, dva, attnb, grads,
                     st2, st3, colt, rowt, s2s, s2r, s3s, s3r, t2s, t2r, t3s, t3r):
    me = lax.axis_index("sp")
    member = me % N4
    base = me - member
    peers = [None, base + (member + 1 - 2 * (member % 2)), base + (member + 2 - N4 * (member // 2)), base + 3 - member]

    barrier = pltpu.get_barrier_semaphore()
    for p in peers[1:]:
        pl.semaphore_signal(barrier, inc=1, device_id={"sp": p}, device_id_type=MESH)

    ri = lax.broadcasted_iota(jnp.int32, (N256, N256), 0)
    ci = lax.broadcasted_iota(jnp.int32, (N256, N256), 1)

    def token_of(i):
        blk = i >> 5
        return ((i & 31) << 3) + ((blk & 1) << 2) + (blk & 2) + (blk >> 2)

    one = jnp.ones((), F32)
    zero = jnp.zeros((), F32)
    perm = jnp.where(token_of(ri) == ci, one, zero).astype(BF16)
    for s in range(2):
        rows = slice(N256 * s, N256 * s + N256)
        xp[rows, :] = dot(perm, x_ref[rows, :]).astype(BF16)
        dyp[rows, :] = dot(perm, dy_ref[rows, :]).astype(BF16)

    low = lanes_low(N512)
    keep = [jnp.where(low, one, zero).astype(BF16), jnp.where(low, zero, one).astype(BF16)]

    for half in range(2):
        cols = slice(N256 * half, N256 * half + N256)
        qq = dot(xp[...], wq_ref[:, cols]).astype(BF16) * jnp.asarray(HEAD_DIM ** -0.5, BF16)
        kk = dot(xp[...], wk_ref[:, cols]).astype(BF16)
        vv = dot(xp[...], wv_ref[:, cols]).astype(BF16)
        dd = dot(dyp[...], wo_ref[cols, :], NT).astype(BF16)
        for u in range(2):
            t = 2 * half + u
            lanes = slice(N128 * u, N128 * u + N128)
            kt[t] = kk[:, lanes]
            vt[t] = vv[:, lanes]
            for par in range(2):
                qm[par, t] = qq[:, lanes] * keep[par]
                dom[par, t] = dd[:, lanes] * keep[par]
            for g, n, off in ((g2, N64, N64 * (t & 1)), (g3, N32, N32 * (2 * (t & 1) + (t >> 1)))):
                for a, ref in ((0, kk), (1, vv)):
                    for s in range(2):
                        r = N256 * s + off
                        g[a, t, n * s:n * s + n, :] = ref[r:r + n, lanes] * keep[0][:n] + ref[r + N128:r + N128 + n, lanes] * keep[1][:n]
                for a, ref in ((2, qq), (3, dd)):
                    for s in range(2):
                        r = N256 * s + off
                        g[a, t, n * s:n * s + n, :] = ref[r:r + n, lanes] * keep[0][:n] + ref[r + N128:r + N128 + n, lanes] * keep[1][:n]

    pl.semaphore_wait(barrier, 3)
    copies2 = []
    copies3 = []
    for a in range(N4):
        c = pltpu.make_async_remote_copy(src_ref=g2.at[a, :, pl.ds(0, N128), :], dst_ref=g2.at[a, :, pl.ds(N128, N128), :],
                                         send_sem=s2s.at[a], recv_sem=s2r.at[a], device_id={"sp": peers[1]}, device_id_type=MESH)
        c.start()
        copies2.append(c)
    for a in range(N4):
        row = []
        for d in (2, 3, 1):
            c = pltpu.make_async_remote_copy(src_ref=g3.at[a, :, pl.ds(0, N64), :], dst_ref=g3.at[a, :, pl.ds(N64 * d, N64), :],
                                             send_sem=s3s.at[a, d], recv_sem=s3r.at[a, d], device_id={"sp": peers[d]}, device_id_type=MESH)
            c.start()
            row.append(c)
        copies3.append(row)

    def forward(q, k, v):
        s = dot(q, k, NT)
        m = jnp.max(s, axis=1, keepdims=True)
        e = jnp.exp(s - m)
        l = jnp.sum(e, axis=1, keepdims=True)
        o = dot(e.astype(BF16), v)
        n = q.shape[0]
        return jnp.broadcast_to(m, (n, N128)), jnp.broadcast_to(l, (n, N128)), o, e

    def merge(t, par, start, n, m, l, o):
        m0 = two(mh, (t, par), start, n)
        l0 = two(lh, (t, par), start, n)
        o0 = two(oh, (t, par), start, n)
        mn = jnp.maximum(m0, m)
        a = jnp.exp(m0 - mn)
        b = jnp.exp(m - mn)
        put_two(mh, (t, par), start, n, mn)
        put_two(lh, (t, par), start, n, l0 * a + l * b)
        put_two(oh, (t, par), start, n, o0 * a + o * b)

    def off2(t, par):
        return pl.multiple_of(N128 * par + N64 * (t % 2), N64)

    def off3(t, par):
        return pl.multiple_of(N128 * par + N64 * (t % 2) + N32 * (t // 2), N32)

    def fwd_local(t, carry):
        for par in range(2):
            for s in range(2):
                rows = slice(N256 * s, N256 * s + N256)
                m, l, o, e = forward(qm[par, t, rows, :], kt[t, rows, :], vt[t, rows, :])
                mh[t, par, rows, :] = m
                lh[t, par, rows, :] = l
                oh[t, par, rows, :] = o
                ms[t, par, rows, :] = m
                est[t, par, rows, :] = e
            m, l, o, e = forward(two(qm, (par, t), N128 * par, N128), two(kt, (t,), N128 * par, N128), two(vt, (t,), N128 * par, N128))
            ms[t, par, N512:N768, :] = m
            est[t, par, N512:N768, :] = e
            merge(t, par, N128 * par, N128, m, l, o)
        return carry

    lax.fori_loop(0, N4, fwd_local, 0)

    for a in range(2):
        copies2[a].wait_recv()
        for c in copies3[a]:
            c.wait_recv()

    low256 = lanes_low(N256)
    colt[...] = jnp.zeros_like(colt)

    def fwd_group(t, carry):
        atts = []
        for par in range(2):
            o2 = off2(t, par)
            m, l, o, e = forward(two(qm, (par, t), o2, N64), g2[0, t], g2[1, t])
            ms[t, par, N768:N896, :] = m
            est[t, par, N768:N896, :] = e
            merge(t, par, o2, N64, m, l, o)
            o3 = off3(t, par)
            m, l, o, e = forward(two(qm, (par, t), o3, N32), g3[0, t], g3[1, t])
            ms[t, par, N896:960, :] = m
            est[t, par, N896:960, :] = e
            merge(t, par, o3, N32, m, l, o)
            lt = lh[t, par]
            att = oh[t, par] / lt
            lse = mh[t, par] + jnp.log(lt)
            delta = jnp.broadcast_to(jnp.sum(dom[par, t].astype(F32) * att, axis=1, keepdims=True), (N512, N128))
            lseh[t, par] = lse
            delh[t, par] = delta
            atts.append(att)
            h = 2 * t + par
            lane = lax.broadcasted_iota(jnp.int32, (N512, N128), 1)
            colt[0:N512, :] = jnp.where(lane == h, lse, jnp.where(lane == h + N8, delta, colt[0:N512, :]))
            l2 = two(lseh, (t, par), o2, N64)
            d2 = two(delh, (t, par), o2, N64)
            colt[N512:N640, :] = jnp.where(lane[:N128] == h, l2, jnp.where(lane[:N128] == h + N8, d2, colt[N512:N640, :]))
            l3 = two(lseh, (t, par), o3, N32)
            d3 = two(delh, (t, par), o3, N32)
            l3 = jnp.concatenate([l3, l3], axis=0)
            d3 = jnp.concatenate([d3, d3], axis=0)
            colt[N640:N768, :] = jnp.where(lane[:N128] == h, l3, jnp.where(lane[:N128] == h + N8, d3, colt[N640:N768, :]))
        attnb[:, pl.ds(pl.multiple_of(N128 * t, N128), N128)] = jnp.where(low, atts[0], atts[1]).astype(BF16)
        return carry

    lax.fori_loop(0, N4, fwd_group, 0)

    st2[0] = jnp.transpose(colt[N512:N640, :])[:N16]
    st3[0] = jnp.transpose(colt[N640:N768, :])[:N16]
    for j in range(N4):
        r = jnp.transpose(colt[N128 * j:N128 * j + N128, :])
        rowt[:, N128 * j:N128 * j + N128] = r[:N16]
    stat2 = pltpu.make_async_remote_copy(src_ref=st2.at[0], dst_ref=st2.at[1], send_sem=t2s, recv_sem=t2r,
                                         device_id={"sp": peers[1]}, device_id_type=MESH)
    stat2.start()
    stats3 = []
    for d in (2, 3, 1):
        c = pltpu.make_async_remote_copy(src_ref=st3.at[0], dst_ref=st3.at[d], send_sem=t3s.at[d], recv_sem=t3r.at[d],
                                         device_id={"sp": peers[d]}, device_id_type=MESH)
        c.start()
        stats3.append(c)

    yb = dot(attnb[...], wo_ref[...]).astype(BF16)
    for s in range(2):
        rows = slice(N256 * s, N256 * s + N256)
        y_ref[rows, :] = dot(perm, yb[rows, :], TN).astype(BF16)
    for t in range(N4):
        g = dot(attnb[:, N128 * t:N128 * t + N128], dyp[...], TN)
        for j in range(N4):
            dw_ref[t, 1536 + N128 * j:1664 + N128 * j, :] = g[:, N128 * j:N128 * j + N128]

    def grad_q(d_rows, k, v, e, delta):
        dp = dot(d_rows, v, NT)
        ds = (e * (dp - wide(delta))).astype(BF16)
        return dot(ds, k)

    def grad_kv(q, d_rows, k, v, lse_row, delta_row):
        st = dot(k, q, NT)
        pt = jnp.exp(st - lse_row)
        dpt = dot(v, d_rows, NT)
        dst = (pt * (dpt - delta_row)).astype(BF16)
        return dot(dst, q), dot(pt.astype(BF16), d_rows)

    def row_of(ref, lead, i):
        return ref[lead + (pl.ds(i, 1), slice(None))]

    def bwd_local(t, carry):
        for par in range(2):
            h = 2 * t + par
            lse_row = row_of(rowt, (), h)
            del_row = row_of(rowt, (), h + N8)
            for s in range(2):
                rows = slice(N256 * s, N256 * s + N256)
                dr = dom[par, t, rows, :]
                kr = kt[t, rows, :]
                vr = vt[t, rows, :]
                lse = lseh[t, par, rows, :]
                dqj = grad_q(dr, kr, vr, est[t, par, rows, :], delh[t, par, rows, :])
                dqh[par, rows, :] = dqj * jnp.exp(ms[t, par, rows, :] - lse)
                gk, gv = grad_kv(qm[par, t, rows, :], dr, kr, vr, lse_row[:, rows], del_row[:, rows])
                if par == 0:
                    dka[t, rows, :] = gk
                    dva[t, rows, :] = gv
                else:
                    dka[t, rows, :] += gk
                    dva[t, rows, :] += gv
            a = N128 * par
            dr = two(dom, (par, t), a, N128)
            kr = two(kt, (t,), a, N128)
            vr = two(vt, (t,), a, N128)
            f = jnp.exp(ms[t, par, N512:N768, :] - two(lseh, (t, par), a, N128))
            dqj = f * grad_q(dr, kr, vr, est[t, par, N512:N768, :], two(delh, (t, par), a, N128))
            put_two(dqh, (par,), a, N128, two(dqh, (par,), a, N128) + dqj)
            lr = jnp.concatenate([lse_row[:, a:a + N128], lse_row[:, N256 + a:N256 + a + N128]], axis=1)
            dlr = jnp.concatenate([del_row[:, a:a + N128], del_row[:, N256 + a:N256 + a + N128]], axis=1)
            gk, gv = grad_kv(two(qm, (par, t), a, N128), dr, kr, vr, lr, dlr)
            put_two(dka, (t,), a, N128, two(dka, (t,), a, N128) + gk)
            put_two(dva, (t,), a, N128, two(dva, (t,), a, N128) + gv)
            for lo, n, off, g in ((N768, N64, off2(t, par), g2), (N896, N32, off3(t, par), g3)):
                f = jnp.exp(ms[t, par, lo:lo + 2 * n, :] - two(lseh, (t, par), off, n))
                dqj = f * grad_q(two(dom, (par, t), off, n), g[0, t], g[1, t], est[t, par, lo:lo + 2 * n, :], two(delh, (t, par), off, n))
                put_two(dqh, (par,), off, n, two(dqh, (par,), off, n) + dqj)
        dq = jnp.where(low, dqh[0], dqh[1]) * (HEAD_DIM ** -0.5)
        grads[0, :, pl.ds(pl.multiple_of(N128 * t, N128), N128)] = dq.astype(BF16)
        return carry

    lax.fori_loop(0, N4, bwd_local, 0)

    stat2.wait_recv()
    for c in stats3:
        c.wait_recv()
    for a in (2, 3):
        copies2[a].wait_recv()
        for c in copies3[a]:
            c.wait_recv()

    keep256 = [keep[0][:N256], keep[1][:N256]]

    def bwd_group(t, carry):
        for par in range(2):
            h = 2 * t + par
            lr = jnp.concatenate([row_of(st2, (0,), h), row_of(st2, (1,), h)], axis=1)
            dlr = jnp.concatenate([row_of(st2, (0,), h + N8), row_of(st2, (1,), h + N8)], axis=1)
            off = off2(t, par)
            gk, gv = grad_kv(g2[2, t] * keep256[par], g2[3, t] * keep256[par], two(kt, (t,), off, N64), two(vt, (t,), off, N64), lr, dlr)
            put_two(dka, (t,), off, N64, two(dka, (t,), off, N64) + gk)
            put_two(dva, (t,), off, N64, two(dva, (t,), off, N64) + gv)
            lo = lax.broadcasted_iota(jnp.int32, (1, N128), 1) < N64
            lr = jnp.concatenate([jnp.where(lo, row_of(st3, (0,), h), row_of(st3, (1,), h)), jnp.where(lo, row_of(st3, (2,), h), row_of(st3, (3,), h))], axis=1)
            dlr = jnp.concatenate([jnp.where(lo, row_of(st3, (0,), h + N8), row_of(st3, (1,), h + N8)), jnp.where(lo, row_of(st3, (2,), h + N8), row_of(st3, (3,), h + N8))], axis=1)
            off = off3(t, par)
            gk, gv = grad_kv(g3[2, t] * keep256[par], g3[3, t] * keep256[par], two(kt, (t,), off, N32), two(vt, (t,), off, N32), lr, dlr)
            put_two(dka, (t,), off, N32, two(dka, (t,), off, N32) + gk)
            put_two(dva, (t,), off, N32, two(dva, (t,), off, N32) + gv)
        cols = pl.ds(pl.multiple_of(N128 * t, N128), N128)
        grads[1, :, cols] = dka[t].astype(BF16)
        grads[2, :, cols] = dva[t].astype(BF16)
        return carry

    lax.fori_loop(0, N4, bwd_group, 0)

    dxb = (dot(grads[0], wq_ref[...], NT) + dot(grads[1], wk_ref[...], NT) + dot(grads[2], wv_ref[...], NT)).astype(BF16)
    for s in range(2):
        rows = slice(N256 * s, N256 * s + N256)
        dx_ref[rows, :] = dot(perm, dxb[rows, :], TN).astype(BF16)
    for i in range(3):
        g = dot(xp[...], grads[i], TN)
        for t in range(N4):
            dw_ref[t, N512 * i:N512 * i + N512, :] = g[:, N128 * t:N128 * t + N128]

    for c in copies2:
        c.wait_send()
    for row in copies3:
        for c in row:
            c.wait_send()
    stat2.wait_send()
    for c in stats3:
        c.wait_send()


def attention(x_loc, w_q, w_k, w_v, w_o, dy_loc):
    vmem = pl.BlockSpec(memory_space=pltpu.VMEM)
    sem = pltpu.SemaphoreType.DMA
    return pl.pallas_call(
        attention_kernel,
        out_shape=[jax.ShapeDtypeStruct((N512, N512), BF16), jax.ShapeDtypeStruct((N512, N512), BF16), jax.ShapeDtypeStruct((N4, 2048, N128), F32)],
        in_specs=[vmem] * 6,
        out_specs=[vmem] * 3,
        scratch_shapes=[
            pltpu.VMEM((N512, N512), BF16), pltpu.VMEM((N512, N512), BF16),
            pltpu.VMEM((2, N4, N512, N128), BF16), pltpu.VMEM((N4, N512, N128), BF16), pltpu.VMEM((N4, N512, N128), BF16), pltpu.VMEM((2, N4, N512, N128), BF16),
            pltpu.VMEM((N4, N4, N256, N128), BF16), pltpu.VMEM((N4, N4, N256, N128), BF16),
            pltpu.VMEM((N4, 2, 960, N256), F32), pltpu.VMEM((N4, 2, 960, N128), F32),
            pltpu.VMEM((N4, 2, N512, N128), F32), pltpu.VMEM((N4, 2, N512, N128), F32), pltpu.VMEM((N4, 2, N512, N128), F32),
            pltpu.VMEM((N4, 2, N512, N128), F32), pltpu.VMEM((N4, 2, N512, N128), F32),
            pltpu.VMEM((2, N512, N128), F32), pltpu.VMEM((N4, N512, N128), F32), pltpu.VMEM((N4, N512, N128), F32),
            pltpu.VMEM((N512, N512), BF16), pltpu.VMEM((3, N512, N512), BF16),
            pltpu.VMEM((2, N16, N128), F32), pltpu.VMEM((N4, N16, N128), F32), pltpu.VMEM((N768, N128), F32), pltpu.VMEM((N16, N512), F32),
            sem((N4,)), sem((N4,)), sem((N4, N4)), sem((N4, N4)), sem, sem, sem((N4,)), sem((N4,)),
        ],
        compiler_params=pltpu.CompilerParams(collective_id=0, has_side_effects=True, vmem_limit_bytes=60 * 2 ** 20),
        name="attention_step",
    )(x_loc, w_q, w_k, w_v, w_o, dy_loc)


COLOR_ROWS = (384, 384, N256)
COLOR_BASE = (0, 384, N768)
STRIDES = (2, N8, N32)


class Reducer:
    def __init__(self, cb, res, pbuf, r1, r2, r3, sems):
        self.cb, self.res, self.pbuf, self.r1, self.r2, self.r3 = cb, res, pbuf, r1, r2, r3
        (self.p0s, self.p0r, self.p1s, self.p1r, self.p2s, self.p2r, self.p3s, self.p3r,
         self.p4s, self.p4r, self.p5s, self.p5r, self.p6s, self.p6r) = sems
        self.me = lax.axis_index("sp")
        self.core = self.me % 2
        self.coord = [(self.me // s) % N4 for s in STRIDES]
        self.mate = self.me + 1 - 2 * self.core

    def peer(self, axis, d):
        return self.me + STRIDES[axis] * ((self.coord[axis] + d) % N4 - self.coord[axis])

    def send(self, src, dst, ss, rs, dev):
        return pltpu.make_async_remote_copy(src_ref=src, dst_ref=dst, send_sem=ss, recv_sem=rs, device_id={"sp": dev}, device_id_type=MESH)

    def half(self, core):
        return pl.ds(pl.multiple_of(N1024 * core, N1024), N1024)

    def rows(self, k, q, p=None):
        n = COLOR_ROWS[k]
        start = N1024 * self.core + COLOR_BASE[k] + (n // N4) * q
        if p is None:
            return pl.ds(pl.multiple_of(start, N8), n // N4)
        return pl.ds(pl.multiple_of(start + (n // N16) * p, N8), n // N16)

    def c0(self, c):
        return self.send(self.cb.at[c, self.half(1 - self.core)], self.pbuf.at[c], self.p0s.at[c], self.p0r.at[c], self.mate)

    def c1(self, c, k, d):
        n = COLOR_ROWS[k] // N4
        a = self.coord[k]
        return self.send(self.cb.at[c, self.rows(k, (a + d) % N4)], self.r1.at[c, k, a, pl.ds(0, n)], self.p1s.at[c, k, d], self.p1r.at[c, k, d], self.peer(k, d))

    def c2(self, c, k, d):
        n = COLOR_ROWS[k] // N16
        b = (k + 1) % 3
        a = self.coord[b]
        src = self.cb.at[c, self.rows(k, self.coord[k], (a + d) % N4)]
        return self.send(src, self.r2.at[c, k, a, pl.ds(0, n)], self.p2s.at[c, k, d], self.p2r.at[c, k, d], self.peer(b, d))

    def c3(self, c, k, d):
        n = COLOR_ROWS[k] // N16
        b = (k + 2) % 3
        a = self.coord[b]
        src = self.cb.at[c, self.rows(k, self.coord[k], self.coord[(k + 1) % 3])]
        return self.send(src, self.r3.at[c, k, a, pl.ds(0, n)], self.p3s.at[c, k, d], self.p3r.at[c, k, d], self.peer(b, d))

    def c4(self, c, k, d):
        b = (k + 1) % 3
        part = self.res.at[c, self.rows(k, self.coord[k], self.coord[b])]
        return self.send(part, part, self.p4s.at[c, k, d], self.p4r.at[c, k, d], self.peer(b, d))

    def c5(self, c, k, d):
        part = self.res.at[c, self.rows(k, self.coord[k])]
        return self.send(part, part, self.p5s.at[c, k, d], self.p5r.at[c, k, d], self.peer(k, d))

    def c6(self, c):
        part = self.res.at[c, self.half(self.core)]
        return self.send(part, part, self.p6s.at[c], self.p6r.at[c], self.mate)

    def each(self, make, c):
        return [make(c, k, d) for d in (1, 3, 2) for k in range(3)]

    def phase(self, i, c):
        core = self.core
        if i == 0:
            self.c0(c).start()
        elif i == 1:
            self.c0(c).wait_recv()
            mine = self.half(core)
            self.cb[c, mine, :] = self.cb[c, mine, :] + self.pbuf[c]
            for x in self.each(self.c1, c):
                x.start()
        elif i == 2:
            for k in range(3):
                for d in (1, 3, 2):
                    self.c1(c, k, d).wait_recv()
                self.total(c, k, self.r1, self.rows(k, self.coord[k]), self.coord[k], COLOR_ROWS[k] // N4, self.cb)
                for d in (1, 3, 2):
                    self.c2(c, k, d).start()
        elif i == 3:
            for k in range(3):
                for d in (1, 3, 2):
                    self.c2(c, k, d).wait_recv()
                b = (k + 1) % 3
                self.total(c, k, self.r2, self.rows(k, self.coord[k], self.coord[b]), self.coord[b], COLOR_ROWS[k] // N16, self.cb)
                for d in (1, 3, 2):
                    self.c3(c, k, d).start()
        elif i == N4:
            for k in range(3):
                for d in (1, 3, 2):
                    self.c3(c, k, d).wait_recv()
                b = (k + 2) % 3
                self.total(c, k, self.r3, self.rows(k, self.coord[k], self.coord[(k + 1) % 3]), self.coord[b], COLOR_ROWS[k] // N16, self.res)
                for d in (1, 3, 2):
                    self.c4(c, k, d).start()
        elif i == 5:
            for k in range(3):
                for d in (1, 3, 2):
                    self.c4(c, k, d).wait_recv()
                for d in (1, 3, 2):
                    self.c5(c, k, d).start()
        elif i == 6:
            for k in range(3):
                for d in (1, 3, 2):
                    self.c5(c, k, d).wait_recv()
            self.c6(c).start()
        elif i == 7:
            self.c6(c).wait_recv()

    def total(self, c, k, slots, rows, a, n, out):
        slots[c, k, a, 0:n, :] = self.cb[c, rows, :]
        out[c, rows, :] = (slots[c, k, 0, 0:n, :] + slots[c, k, 1, 0:n, :]) + (slots[c, k, 2, 0:n, :] + slots[c, k, 3, 0:n, :])

    def finish(self, c):
        self.c0(c).wait_send()
        for make in (self.c1, self.c2, self.c3, self.c4, self.c5):
            for x in self.each(make, c):
                x.wait_send()
        self.c6(c).wait_send()


def reducer_scratch():
    sem = pltpu.SemaphoreType.DMA
    bufs = [pltpu.VMEM((N4, 2048, N128), F32), pltpu.VMEM((N4, N1024, N128), F32), pltpu.VMEM((N4, 3, N4, 96, N128), F32),
            pltpu.VMEM((N4, 3, N4, 24, N128), F32), pltpu.VMEM((N4, 3, N4, 24, N128), F32)]
    sems = [sem((N4,)), sem((N4,))] + [sem((N4, 3, N4))] * 10 + [sem((N4,)), sem((N4,))]
    return bufs, sems


def write_out(res, outs, sem, t):
    copies = []
    cols = pl.ds(pl.multiple_of(N128 * t, N128), N128)
    for i in range(3):
        copies.append(pltpu.make_async_copy(res.at[t, pl.ds(N512 * i, N512)], outs[i].at[:, cols], sem.at[t, i]))
    for j in range(N4):
        copies.append(pltpu.make_async_copy(res.at[t, pl.ds(1536 + N128 * j, N128)], outs[3].at[cols, pl.ds(N128 * j, N128)], sem.at[t, 3 + j]))
    return copies


def reduce_kernel(cb, o0, o1, o2, o3, work, res, pbuf, r1, r2, r3, wsem, *sems):
    red = Reducer(work, res, pbuf, r1, r2, r3, sems)
    barrier = pltpu.get_barrier_semaphore()
    peers = [red.mate] + [red.peer(a, d) for a in range(3) for d in (1, 2, 3)]
    for p in peers:
        pl.semaphore_signal(barrier, inc=1, device_id={"sp": p}, device_id_type=MESH)
    work[...] = cb[...]
    pl.semaphore_wait(barrier, len(peers))
    for i in range(N8):
        for c in range(N4):
            red.phase(i, c)
            if i == 7:
                for x in write_out(res, (o0, o1, o2, o3), wsem, c):
                    x.start()
    for c in range(N4):
        red.finish(c)
        for x in write_out(res, (o0, o1, o2, o3), wsem, c):
            x.wait()


def reduce_grads(chunks):
    vmem = pl.BlockSpec(memory_space=pltpu.VMEM)
    bufs, sems = reducer_scratch()
    return pl.pallas_call(
        reduce_kernel,
        out_shape=[jax.ShapeDtypeStruct((N512, N512), F32)] * N4,
        in_specs=[vmem],
        out_specs=[pl.BlockSpec(memory_space=pl.ANY)] * N4,
        scratch_shapes=[pltpu.VMEM((N4, 2048, N128), F32)] + bufs + [pltpu.SemaphoreType.DMA((N4, 7))] + sems,
        compiler_params=pltpu.CompilerParams(collective_id=1, has_side_effects=True, vmem_limit_bytes=60 * 2 ** 20),
        name="reduce_grads",
    )(chunks)


def solution(mesh):
    def device_step(x_loc, w_q, w_k, w_v, w_o, dy_loc):
        y_loc, dx_loc, dws = attention(x_loc, w_q, w_k, w_v, w_o, dy_loc)
        return y_loc, dx_loc, *reduce_grads(dws)

    row_spec = P(("dp", "sp"), None)
    full_spec = P(None, None)
    grad_spec = P("dp", None)
    return jax.shard_map(device_step, mesh=mesh, in_specs=(row_spec, full_spec, full_spec, full_spec, full_spec, row_spec),
                         out_specs=(row_spec, row_spec, grad_spec, grad_spec, grad_spec, grad_spec), check_vma=False)
```

```python
import functools

import jax
import jax.numpy as jnp
from jax import lax
from jax.experimental import pallas as pl
from jax.experimental.pallas import tpu as pltpu
from jax.sharding import PartitionSpec as P

HEAD_DIM = 64
N4 = 4
N8 = 8
N16 = 16
N32 = 32
N64 = 64
N128 = 128
N256 = 256
N512 = 512
N640 = 640
N768 = 768
N896 = 896
N1024 = 1024
F32 = jnp.float32
BF16 = jnp.bfloat16
MESH = pl.DeviceIdType.MESH
NN = (((1,), (0,)), ((), ()))
NT = (((1,), (1,)), ((), ()))
TN = (((0,), (0,)), ((), ()))


def dot(a, b, dims=NN):
    return lax.dot_general(a, b, dims, preferred_element_type=F32)


def two(ref, lead, start, n):
    return jnp.concatenate([ref[lead + (pl.ds(start, n), slice(None))], ref[lead + (pl.ds(N256 + start, n), slice(None))]], axis=0)


def put_two(ref, lead, start, n, val):
    ref[lead + (pl.ds(start, n), slice(None))] = val[:n]
    ref[lead + (pl.ds(N256 + start, n), slice(None))] = val[n:]


def wide(stat):
    return jnp.concatenate([stat, stat], axis=1)


def lanes_low(rows):
    return lax.broadcasted_iota(jnp.int32, (rows, N128), 1) < N64


COLOR_ROWS = (384, 384, N256)
COLOR_BASE = (0, 384, N768)
STRIDES = (2, N8, N32)


class Reducer:
    def __init__(self, cb, res, pbuf, r1, r2, r3, sems):
        self.cb, self.res, self.pbuf, self.r1, self.r2, self.r3 = cb, res, pbuf, r1, r2, r3
        (self.p0s, self.p0r, self.p1s, self.p1r, self.p2s, self.p2r, self.p3s, self.p3r,
         self.p4s, self.p4r, self.p5s, self.p5r, self.p6s, self.p6r) = sems
        self.me = lax.axis_index("sp")
        self.core = self.me % 2
        self.coord = [(self.me // s) % N4 for s in STRIDES]
        self.mate = self.me + 1 - 2 * self.core

    def peer(self, axis, d):
        return self.me + STRIDES[axis] * ((self.coord[axis] + d) % N4 - self.coord[axis])

    def send(self, src, dst, ss, rs, dev):
        return pltpu.make_async_remote_copy(src_ref=src, dst_ref=dst, send_sem=ss, recv_sem=rs, device_id={"sp": dev}, device_id_type=MESH)

    def half(self, core):
        return pl.ds(pl.multiple_of(N1024 * core, N1024), N1024)

    def rows(self, k, q, p=None):
        n = COLOR_ROWS[k]
        start = N1024 * self.core + COLOR_BASE[k] + (n // N4) * q
        if p is None:
            return pl.ds(pl.multiple_of(start, N8), n // N4)
        return pl.ds(pl.multiple_of(start + (n // N16) * p, N8), n // N16)

    def c0(self, c):
        return self.send(self.cb.at[c, self.half(1 - self.core)], self.pbuf.at[c], self.p0s.at[c], self.p0r.at[c], self.mate)

    def c1(self, c, k, d):
        n = COLOR_ROWS[k] // N4
        a = self.coord[k]
        return self.send(self.cb.at[c, self.rows(k, (a + d) % N4)], self.r1.at[c, k, a, pl.ds(0, n)], self.p1s.at[c, k, d], self.p1r.at[c, k, d], self.peer(k, d))

    def c2(self, c, k, d):
        n = COLOR_ROWS[k] // N16
        b = (k + 1) % 3
        a = self.coord[b]
        src = self.cb.at[c, self.rows(k, self.coord[k], (a + d) % N4)]
        return self.send(src, self.r2.at[c, k, a, pl.ds(0, n)], self.p2s.at[c, k, d], self.p2r.at[c, k, d], self.peer(b, d))

    def c3(self, c, k, d):
        n = COLOR_ROWS[k] // N16
        b = (k + 2) % 3
        a = self.coord[b]
        src = self.cb.at[c, self.rows(k, self.coord[k], self.coord[(k + 1) % 3])]
        return self.send(src, self.r3.at[c, k, a, pl.ds(0, n)], self.p3s.at[c, k, d], self.p3r.at[c, k, d], self.peer(b, d))

    def c4(self, c, k, d):
        b = (k + 1) % 3
        part = self.res.at[c, self.rows(k, self.coord[k], self.coord[b])]
        return self.send(part, part, self.p4s.at[c, k, d], self.p4r.at[c, k, d], self.peer(b, d))

    def c5(self, c, k, d):
        part = self.res.at[c, self.rows(k, self.coord[k])]
        return self.send(part, part, self.p5s.at[c, k, d], self.p5r.at[c, k, d], self.peer(k, d))

    def c6(self, c):
        part = self.res.at[c, self.half(self.core)]
        return self.send(part, part, self.p6s.at[c], self.p6r.at[c], self.mate)

    def each(self, make, c):
        return [make(c, k, d) for d in (1, 3, 2) for k in range(3)]

    def phase(self, i, c):
        core = self.core
        if i == 0:
            self.c0(c).start()
        elif i == 1:
            self.c0(c).wait_recv()
            mine = self.half(core)
            self.cb[c, mine, :] = self.cb[c, mine, :] + self.pbuf[c]
            for x in self.each(self.c1, c):
                x.start()
        elif i == 2:
            for k in range(3):
                for d in (1, 3, 2):
                    self.c1(c, k, d).wait_recv()
                self.total(c, k, self.r1, self.rows(k, self.coord[k]), self.coord[k], COLOR_ROWS[k] // N4, self.cb)
                for d in (1, 3, 2):
                    self.c2(c, k, d).start()
        elif i == 3:
            for k in range(3):
                for d in (1, 3, 2):
                    self.c2(c, k, d).wait_recv()
                b = (k + 1) % 3
                self.total(c, k, self.r2, self.rows(k, self.coord[k], self.coord[b]), self.coord[b], COLOR_ROWS[k] // N16, self.cb)
                for d in (1, 3, 2):
                    self.c3(c, k, d).start()
        elif i == N4:
            for k in range(3):
                for d in (1, 3, 2):
                    self.c3(c, k, d).wait_recv()
                b = (k + 2) % 3
                self.total(c, k, self.r3, self.rows(k, self.coord[k], self.coord[(k + 1) % 3]), self.coord[b], COLOR_ROWS[k] // N16, self.res)
                for d in (1, 3, 2):
                    self.c4(c, k, d).start()
        elif i == 5:
            for k in range(3):
                for d in (1, 3, 2):
                    self.c4(c, k, d).wait_recv()
                for d in (1, 3, 2):
                    self.c5(c, k, d).start()
        elif i == 6:
            for k in range(3):
                for d in (1, 3, 2):
                    self.c5(c, k, d).wait_recv()
            self.c6(c).start()
        elif i == 7:
            self.c6(c).wait_recv()

    def total(self, c, k, slots, rows, a, n, out):
        slots[c, k, a, 0:n, :] = self.cb[c, rows, :]
        out[c, rows, :] = (slots[c, k, 0, 0:n, :] + slots[c, k, 1, 0:n, :]) + (slots[c, k, 2, 0:n, :] + slots[c, k, 3, 0:n, :])

    def finish(self, c):
        self.c0(c).wait_send()
        for make in (self.c1, self.c2, self.c3, self.c4, self.c5):
            for x in self.each(make, c):
                x.wait_send()
        self.c6(c).wait_send()


def reducer_scratch():
    sem = pltpu.SemaphoreType.DMA
    bufs = [pltpu.VMEM((N4, 2048, N128), F32), pltpu.VMEM((N4, N1024, N128), F32), pltpu.VMEM((N4, 3, N4, 96, N128), F32),
            pltpu.VMEM((N4, 3, N4, 24, N128), F32), pltpu.VMEM((N4, 3, N4, 24, N128), F32)]
    sems = [sem((N4,)), sem((N4,))] + [sem((N4, 3, N4))] * 10 + [sem((N4,)), sem((N4,))]
    return bufs, sems


def write_out(res, outs, sem, t):
    copies = []
    cols = pl.ds(pl.multiple_of(N128 * t, N128), N128)
    for i in range(3):
        copies.append(pltpu.make_async_copy(res.at[t, pl.ds(N512 * i, N512)], outs[i].at[:, cols], sem.at[t, i]))
    for j in range(N4):
        copies.append(pltpu.make_async_copy(res.at[t, pl.ds(1536 + N128 * j, N128)], outs[3].at[cols, pl.ds(N128 * j, N128)], sem.at[t, 3 + j]))
    return copies


def attention_kernel(x_ref, wq_ref, wk_ref, wv_ref, wo_ref, dy_ref, y_hbm, dx_hbm, o0, o1, o2, o3,
                     xp, dyp, qm, kt, vt, dom, g2, g3, est, ms, mh, lh, oh, lseh, delh, dqh, dka, dva, attnb, grads,
                     st2, st3, colt, rowt, s2s, s2r, s3s, s3r, t2s, t2r, t3s, t3r, y_ref, dx_ref, cb, res, pbuf, r1, r2, r3, wsem, osem, *rsems):
    red = Reducer(cb, res, pbuf, r1, r2, r3, rsems)
    me = lax.axis_index("sp")
    member = me % N4
    base = me - member
    peers = [None, base + (member + 1 - 2 * (member % 2)), base + (member + 2 - N4 * (member // 2)), base + 3 - member]

    barrier = pltpu.get_barrier_semaphore()
    everyone = [peers[1], peers[3]] + [red.peer(ax, d) for ax in range(3) for d in (1, 2, 3)]
    for p in everyone:
        pl.semaphore_signal(barrier, inc=1, device_id={"sp": p}, device_id_type=MESH)

    ri = lax.broadcasted_iota(jnp.int32, (N256, N256), 0)
    ci = lax.broadcasted_iota(jnp.int32, (N256, N256), 1)

    def token_of(i):
        blk = i >> 5
        return ((i & 31) << 3) + ((blk & 1) << 2) + (blk & 2) + (blk >> 2)

    one = jnp.ones((), F32)
    zero = jnp.zeros((), F32)
    perm = jnp.where(token_of(ri) == ci, one, zero).astype(BF16)
    for s in range(2):
        rows = slice(N256 * s, N256 * s + N256)
        xp[rows, :] = dot(perm, x_ref[rows, :]).astype(BF16)
        dyp[rows, :] = dot(perm, dy_ref[rows, :]).astype(BF16)

    low = lanes_low(N512)
    keep = [jnp.where(low, one, zero).astype(BF16), jnp.where(low, zero, one).astype(BF16)]

    for half in range(2):
        cols = slice(N256 * half, N256 * half + N256)
        qq = dot(xp[...], wq_ref[:, cols]).astype(BF16) * jnp.asarray(HEAD_DIM ** -0.5, BF16)
        kk = dot(xp[...], wk_ref[:, cols]).astype(BF16)
        vv = dot(xp[...], wv_ref[:, cols]).astype(BF16)
        dd = dot(dyp[...], wo_ref[cols, :], NT).astype(BF16)
        for u in range(2):
            t = 2 * half + u
            lanes = slice(N128 * u, N128 * u + N128)
            kt[t] = kk[:, lanes]
            vt[t] = vv[:, lanes]
            for par in range(2):
                qm[par, t] = qq[:, lanes] * keep[par]
                dom[par, t] = dd[:, lanes] * keep[par]
            for g, n, off in ((g2, N64, N64 * (t & 1)), (g3, N32, N32 * (2 * (t & 1) + (t >> 1)))):
                for a, ref in ((0, kk), (1, vv)):
                    for s in range(2):
                        r = N256 * s + off
                        g[a, t, n * s:n * s + n, :] = ref[r:r + n, lanes] * keep[0][:n] + ref[r + N128:r + N128 + n, lanes] * keep[1][:n]
                for a, ref in ((2, qq), (3, dd)):
                    for s in range(2):
                        r = N256 * s + off
                        g[a, t, n * s:n * s + n, :] = ref[r:r + n, lanes] * keep[0][:n] + ref[r + N128:r + N128 + n, lanes] * keep[1][:n]

    pl.semaphore_wait(barrier, len(everyone))
    copies2 = []
    copies3 = []
    for a in range(N4):
        c = pltpu.make_async_remote_copy(src_ref=g2.at[a, :, pl.ds(0, N128), :], dst_ref=g2.at[a, :, pl.ds(N128, N128), :],
                                         send_sem=s2s.at[a], recv_sem=s2r.at[a], device_id={"sp": peers[1]}, device_id_type=MESH)
        c.start()
        copies2.append(c)
    for a in range(N4):
        row = []
        for d in (2, 3, 1):
            c = pltpu.make_async_remote_copy(src_ref=g3.at[a, :, pl.ds(0, N64), :], dst_ref=g3.at[a, :, pl.ds(N64 * d, N64), :],
                                             send_sem=s3s.at[a, d], recv_sem=s3r.at[a, d], device_id={"sp": peers[d]}, device_id_type=MESH)
            c.start()
            row.append(c)
        copies3.append(row)

    def forward(q, k, v):
        s = dot(q, k, NT)
        m = jnp.max(s, axis=1, keepdims=True)
        e = jnp.exp(s - m)
        l = jnp.sum(e, axis=1, keepdims=True)
        o = dot(e.astype(BF16), v)
        n = q.shape[0]
        return jnp.broadcast_to(m, (n, N128)), jnp.broadcast_to(l, (n, N128)), o, e

    def merge(t, par, start, n, m, l, o):
        m0 = two(mh, (t, par), start, n)
        l0 = two(lh, (t, par), start, n)
        o0 = two(oh, (t, par), start, n)
        mn = jnp.maximum(m0, m)
        a = jnp.exp(m0 - mn)
        b = jnp.exp(m - mn)
        put_two(mh, (t, par), start, n, mn)
        put_two(lh, (t, par), start, n, l0 * a + l * b)
        put_two(oh, (t, par), start, n, o0 * a + o * b)

    def off2(t, par):
        return pl.multiple_of(N128 * par + N64 * (t % 2), N64)

    def off3(t, par):
        return pl.multiple_of(N128 * par + N64 * (t % 2) + N32 * (t // 2), N32)

    def fwd_local(t, carry):
        for par in range(2):
            for s in range(2):
                rows = slice(N256 * s, N256 * s + N256)
                m, l, o, e = forward(qm[par, t, rows, :], kt[t, rows, :], vt[t, rows, :])
                mh[t, par, rows, :] = m
                lh[t, par, rows, :] = l
                oh[t, par, rows, :] = o
                ms[t, par, rows, :] = m
                est[t, par, rows, :] = e
            m, l, o, e = forward(two(qm, (par, t), N128 * par, N128), two(kt, (t,), N128 * par, N128), two(vt, (t,), N128 * par, N128))
            ms[t, par, N512:N768, :] = m
            est[t, par, N512:N768, :] = e
            merge(t, par, N128 * par, N128, m, l, o)
        return carry

    lax.fori_loop(0, N4, fwd_local, 0)

    for a in range(2):
        copies2[a].wait_recv()
        for c in copies3[a]:
            c.wait_recv()

    low256 = lanes_low(N256)
    colt[...] = jnp.zeros_like(colt)

    def fwd_group(t, carry):
        atts = []
        for par in range(2):
            o2 = off2(t, par)
            m, l, o, e = forward(two(qm, (par, t), o2, N64), g2[0, t], g2[1, t])
            ms[t, par, N768:N896, :] = m
            est[t, par, N768:N896, :] = e
            merge(t, par, o2, N64, m, l, o)
            o3 = off3(t, par)
            m, l, o, e = forward(two(qm, (par, t), o3, N32), g3[0, t], g3[1, t])
            ms[t, par, N896:960, :] = m
            est[t, par, N896:960, :] = e
            merge(t, par, o3, N32, m, l, o)
            lt = lh[t, par]
            att = oh[t, par] / lt
            lse = mh[t, par] + jnp.log(lt)
            delta = jnp.broadcast_to(jnp.sum(dom[par, t].astype(F32) * att, axis=1, keepdims=True), (N512, N128))
            lseh[t, par] = lse
            delh[t, par] = delta
            atts.append(att)
            h = 2 * t + par
            lane = lax.broadcasted_iota(jnp.int32, (N512, N128), 1)
            colt[0:N512, :] = jnp.where(lane == h, lse, jnp.where(lane == h + N8, delta, colt[0:N512, :]))
            l2 = two(lseh, (t, par), o2, N64)
            d2 = two(delh, (t, par), o2, N64)
            colt[N512:N640, :] = jnp.where(lane[:N128] == h, l2, jnp.where(lane[:N128] == h + N8, d2, colt[N512:N640, :]))
            l3 = two(lseh, (t, par), o3, N32)
            d3 = two(delh, (t, par), o3, N32)
            l3 = jnp.concatenate([l3, l3], axis=0)
            d3 = jnp.concatenate([d3, d3], axis=0)
            colt[N640:N768, :] = jnp.where(lane[:N128] == h, l3, jnp.where(lane[:N128] == h + N8, d3, colt[N640:N768, :]))
        attnb[:, pl.ds(pl.multiple_of(N128 * t, N128), N128)] = jnp.where(low, atts[0], atts[1]).astype(BF16)
        return carry

    lax.fori_loop(0, N4, fwd_group, 0)

    st2[0] = jnp.transpose(colt[N512:N640, :])[:N16]
    st3[0] = jnp.transpose(colt[N640:N768, :])[:N16]
    for j in range(N4):
        r = jnp.transpose(colt[N128 * j:N128 * j + N128, :])
        rowt[:, N128 * j:N128 * j + N128] = r[:N16]
    stat2 = pltpu.make_async_remote_copy(src_ref=st2.at[0], dst_ref=st2.at[1], send_sem=t2s, recv_sem=t2r,
                                         device_id={"sp": peers[1]}, device_id_type=MESH)
    stat2.start()
    stats3 = []
    for d in (2, 3, 1):
        c = pltpu.make_async_remote_copy(src_ref=st3.at[0], dst_ref=st3.at[d], send_sem=t3s.at[d], recv_sem=t3r.at[d],
                                         device_id={"sp": peers[d]}, device_id_type=MESH)
        c.start()
        stats3.append(c)

    def grad_q(d_rows, k, v, e, delta):
        dp = dot(d_rows, v, NT)
        ds = (e * (dp - wide(delta))).astype(BF16)
        return dot(ds, k)

    def grad_kv(q, d_rows, k, v, lse_row, delta_row):
        st = dot(k, q, NT)
        pt = jnp.exp(st - lse_row)
        dpt = dot(v, d_rows, NT)
        dst = (pt * (dpt - delta_row)).astype(BF16)
        return dot(dst, q), dot(pt.astype(BF16), d_rows)

    def row_of(ref, lead, i):
        return ref[lead + (pl.ds(i, 1), slice(None))]

    def bwd_local(t, par):
        if True:
            h = 2 * t + par
            lse_row = row_of(rowt, (), h)
            del_row = row_of(rowt, (), h + N8)
            for s in range(2):
                rows = slice(N256 * s, N256 * s + N256)
                dr = dom[par, t, rows, :]
                kr = kt[t, rows, :]
                vr = vt[t, rows, :]
                lse = lseh[t, par, rows, :]
                dqj = grad_q(dr, kr, vr, est[t, par, rows, :], delh[t, par, rows, :])
                dqh[par, rows, :] = dqj * jnp.exp(ms[t, par, rows, :] - lse)
                gk, gv = grad_kv(qm[par, t, rows, :], dr, kr, vr, lse_row[:, rows], del_row[:, rows])
                if par == 0:
                    dka[t, rows, :] = gk
                    dva[t, rows, :] = gv
                else:
                    dka[t, rows, :] += gk
                    dva[t, rows, :] += gv
            a = N128 * par
            dr = two(dom, (par, t), a, N128)
            kr = two(kt, (t,), a, N128)
            vr = two(vt, (t,), a, N128)
            f = jnp.exp(ms[t, par, N512:N768, :] - two(lseh, (t, par), a, N128))
            dqj = f * grad_q(dr, kr, vr, est[t, par, N512:N768, :], two(delh, (t, par), a, N128))
            put_two(dqh, (par,), a, N128, two(dqh, (par,), a, N128) + dqj)
            lr = jnp.concatenate([lse_row[:, a:a + N128], lse_row[:, N256 + a:N256 + a + N128]], axis=1)
            dlr = jnp.concatenate([del_row[:, a:a + N128], del_row[:, N256 + a:N256 + a + N128]], axis=1)
            gk, gv = grad_kv(two(qm, (par, t), a, N128), dr, kr, vr, lr, dlr)
            put_two(dka, (t,), a, N128, two(dka, (t,), a, N128) + gk)
            put_two(dva, (t,), a, N128, two(dva, (t,), a, N128) + gv)
            for lo, n, off, g in ((N768, N64, off2(t, par), g2), (N896, N32, off3(t, par), g3)):
                f = jnp.exp(ms[t, par, lo:lo + 2 * n, :] - two(lseh, (t, par), off, n))
                dqj = f * grad_q(two(dom, (par, t), off, n), g[0, t], g[1, t], est[t, par, lo:lo + 2 * n, :], two(delh, (t, par), off, n))
                put_two(dqh, (par,), off, n, two(dqh, (par,), off, n) + dqj)

    keep256 = [keep[0][:N256], keep[1][:N256]]

    def bwd_group(t, par):
        if True:
            h = 2 * t + par
            lr = jnp.concatenate([row_of(st2, (0,), h), row_of(st2, (1,), h)], axis=1)
            dlr = jnp.concatenate([row_of(st2, (0,), h + N8), row_of(st2, (1,), h + N8)], axis=1)
            off = off2(t, par)
            gk, gv = grad_kv(g2[2, t] * keep256[par], g2[3, t] * keep256[par], two(kt, (t,), off, N64), two(vt, (t,), off, N64), lr, dlr)
            put_two(dka, (t,), off, N64, two(dka, (t,), off, N64) + gk)
            put_two(dva, (t,), off, N64, two(dva, (t,), off, N64) + gv)
            lo = lax.broadcasted_iota(jnp.int32, (1, N128), 1) < N64
            lr = jnp.concatenate([jnp.where(lo, row_of(st3, (0,), h), row_of(st3, (1,), h)), jnp.where(lo, row_of(st3, (2,), h), row_of(st3, (3,), h))], axis=1)
            dlr = jnp.concatenate([jnp.where(lo, row_of(st3, (0,), h + N8), row_of(st3, (1,), h + N8)), jnp.where(lo, row_of(st3, (2,), h + N8), row_of(st3, (3,), h + N8))], axis=1)
            off = off3(t, par)
            gk, gv = grad_kv(g3[2, t] * keep256[par], g3[3, t] * keep256[par], two(kt, (t,), off, N32), two(vt, (t,), off, N32), lr, dlr)
            put_two(dka, (t,), off, N32, two(dka, (t,), off, N32) + gk)
            put_two(dva, (t,), off, N32, two(dva, (t,), off, N32) + gv)

    def chunk(t):
        cols = slice(N128 * t, N128 * t + N128)
        dq = jnp.where(low, dqh[0], dqh[1]) * (HEAD_DIM ** -0.5)
        for i, g in enumerate((dq, dka[t], dva[t])):
            gb = g.astype(BF16)
            grads[i, :, cols] = gb
            cb[t, N512 * i:N512 * i + N512, :] = dot(xp[...], gb, TN)
        g = dot(attnb[:, cols], dyp[...], TN)
        for j in range(N4):
            cb[t, 1536 + N128 * j:1664 + N128 * j, :] = g[:, N128 * j:N128 * j + N128]

    def step(t, lag):
        for c in range(t + 1):
            i = lag - 2 * c
            if 0 <= i <= 7:
                red.phase(i, c)
                if i == 7:
                    for x in write_out(res, (o0, o1, o2, o3), wsem, c):
                        x.start()

    for t in range(N4):
        bwd_local(t, 0)
        bwd_local(t, 1)
        step(t - 1, 2 * t - 1)
        if t == 0:
            stat2.wait_recv()
            for c in stats3:
                c.wait_recv()
            for a in (2, 3):
                copies2[a].wait_recv()
                for c in copies3[a]:
                    c.wait_recv()
        bwd_group(t, 0)
        bwd_group(t, 1)
        chunk(t)
        step(t, 2 * t)

    def y_part(s):
        rows = slice(N256 * s, N256 * s + N256)
        yb = dot(attnb[rows, :], wo_ref[...]).astype(BF16)
        y_ref[rows, :] = dot(perm, yb, TN).astype(BF16)

    def dx_part(s):
        rows = slice(N256 * s, N256 * s + N256)
        dxb = (dot(grads[0, rows, :], wq_ref[...], NT) + dot(grads[1, rows, :], wk_ref[...], NT) + dot(grads[2, rows, :], wv_ref[...], NT)).astype(BF16)
        dx_ref[rows, :] = dot(perm, dxb, TN).astype(BF16)

    y_out = pltpu.make_async_copy(y_ref, y_hbm, osem.at[0])
    dx_out = pltpu.make_async_copy(dx_ref, dx_hbm, osem.at[1])
    work = [functools.partial(dx_part, 0), functools.partial(dx_part, 1), functools.partial(y_part, 0), functools.partial(y_part, 1)]
    for lag in range(7, 14):
        if work:
            work.pop(0)()
        elif lag == 11:
            y_out.start()
            dx_out.start()
        step(3, lag)

    for c in copies2:
        c.wait_send()
    for row in copies3:
        for c in row:
            c.wait_send()
    stat2.wait_send()
    for c in stats3:
        c.wait_send()
    for c in range(N4):
        red.finish(c)
        for x in write_out(res, (o0, o1, o2, o3), wsem, c):
            x.wait()
    y_out.wait()
    dx_out.wait()


def attention(x_loc, w_q, w_k, w_v, w_o, dy_loc):
    vmem = pl.BlockSpec(memory_space=pltpu.VMEM)
    sem = pltpu.SemaphoreType.DMA
    bufs, sems = reducer_scratch()
    return pl.pallas_call(
        attention_kernel,
        out_shape=[jax.ShapeDtypeStruct((N512, N512), BF16)] * 2 + [jax.ShapeDtypeStruct((N512, N512), F32)] * N4,
        in_specs=[vmem] * 6,
        out_specs=[pl.BlockSpec(memory_space=pl.ANY)] * 6,
        scratch_shapes=[
            pltpu.VMEM((N512, N512), BF16), pltpu.VMEM((N512, N512), BF16),
            pltpu.VMEM((2, N4, N512, N128), BF16), pltpu.VMEM((N4, N512, N128), BF16), pltpu.VMEM((N4, N512, N128), BF16), pltpu.VMEM((2, N4, N512, N128), BF16),
            pltpu.VMEM((N4, N4, N256, N128), BF16), pltpu.VMEM((N4, N4, N256, N128), BF16),
            pltpu.VMEM((N4, 2, 960, N256), F32), pltpu.VMEM((N4, 2, 960, N128), F32),
            pltpu.VMEM((N4, 2, N512, N128), F32), pltpu.VMEM((N4, 2, N512, N128), F32), pltpu.VMEM((N4, 2, N512, N128), F32),
            pltpu.VMEM((N4, 2, N512, N128), F32), pltpu.VMEM((N4, 2, N512, N128), F32),
            pltpu.VMEM((2, N512, N128), F32), pltpu.VMEM((N4, N512, N128), F32), pltpu.VMEM((N4, N512, N128), F32),
            pltpu.VMEM((N512, N512), BF16), pltpu.VMEM((3, N512, N512), BF16),
            pltpu.VMEM((2, N16, N128), F32), pltpu.VMEM((N4, N16, N128), F32), pltpu.VMEM((N768, N128), F32), pltpu.VMEM((N16, N512), F32),
            sem((N4,)), sem((N4,)), sem((N4, N4)), sem((N4, N4)), sem, sem, sem((N4,)), sem((N4,)),
            pltpu.VMEM((N512, N512), BF16), pltpu.VMEM((N512, N512), BF16), pltpu.VMEM((N4, 2048, N128), F32),
        ] + bufs + [sem((N4, 7)), sem((2,))] + sems,
        compiler_params=pltpu.CompilerParams(collective_id=0, has_side_effects=True, vmem_limit_bytes=60 * 2 ** 20),
        name="attention_step",
    )(x_loc, w_q, w_k, w_v, w_o, dy_loc)


def solution(mesh):
    def device_step(x_loc, w_q, w_k, w_v, w_o, dy_loc):
        return tuple(attention(x_loc, w_q, w_k, w_v, w_o, dy_loc))

    row_spec = P(("dp", "sp"), None)
    full_spec = P(None, None)
    grad_spec = P("dp", None)
    return jax.shard_map(device_step, mesh=mesh, in_specs=(row_spec, full_spec, full_spec, full_spec, full_spec, row_spec),
                         out_specs=(row_spec, row_spec, grad_spec, grad_spec, grad_spec, grad_spec), check_vma=False)
```

```python
import functools

import jax
import jax.numpy as jnp
from jax import lax
from jax.experimental import pallas as pl
from jax.experimental.pallas import tpu as pltpu
from jax.sharding import PartitionSpec as P

HEAD_DIM = 64
N4 = 4
N8 = 8
N16 = 16
N32 = 32
N64 = 64
N128 = 128
N256 = 256
N512 = 512
N640 = 640
N768 = 768
N1024 = 1024
F32 = jnp.float32
BF16 = jnp.bfloat16
MESH = pl.DeviceIdType.MESH
NN = (((1,), (0,)), ((), ()))
NT = (((1,), (1,)), ((), ()))
TN = (((0,), (0,)), ((), ()))


def dot(a, b, dims=NN):
    return lax.dot_general(a, b, dims, preferred_element_type=F32)


def two(ref, lead, start, n):
    return jnp.concatenate([ref[lead + (pl.ds(start, n), slice(None))], ref[lead + (pl.ds(N256 + start, n), slice(None))]], axis=0)


def put_two(ref, lead, start, n, val):
    ref[lead + (pl.ds(start, n), slice(None))] = val[:n]
    ref[lead + (pl.ds(N256 + start, n), slice(None))] = val[n:]


def wide(stat):
    return jnp.concatenate([stat, stat], axis=1)


def add_two(ref, lead, start, n, val):
    put_two(ref, lead, start, n, two(ref, lead, start, n) + val)


def lanes_low(rows):
    return lax.broadcasted_iota(jnp.int32, (rows, N128), 1) < N64


COLOR_ROWS = (384, 384, N256)
COLOR_BASE = (0, 384, N768)
STRIDES = (2, N8, N32)


class Reducer:
    def __init__(self, cb, res, pbuf, r1, r2, r3, sems):
        self.cb, self.res, self.pbuf, self.r1, self.r2, self.r3 = cb, res, pbuf, r1, r2, r3
        (self.p0s, self.p0r, self.p1s, self.p1r, self.p2s, self.p2r, self.p3s, self.p3r,
         self.p4s, self.p4r, self.p5s, self.p5r, self.p6s, self.p6r) = sems
        self.me = lax.axis_index("sp")
        self.core = self.me % 2
        self.coord = [(self.me // s) % N4 for s in STRIDES]
        self.mate = self.me + 1 - 2 * self.core

    def peer(self, axis, d):
        return self.me + STRIDES[axis] * ((self.coord[axis] + d) % N4 - self.coord[axis])

    def send(self, src, dst, ss, rs, dev):
        return pltpu.make_async_remote_copy(src_ref=src, dst_ref=dst, send_sem=ss, recv_sem=rs, device_id={"sp": dev}, device_id_type=MESH)

    def half(self, core):
        return pl.ds(pl.multiple_of(N1024 * core, N1024), N1024)

    def rows(self, k, q, p=None):
        n = COLOR_ROWS[k]
        start = N1024 * self.core + COLOR_BASE[k] + (n // N4) * q
        if p is None:
            return pl.ds(pl.multiple_of(start, N8), n // N4)
        return pl.ds(pl.multiple_of(start + (n // N16) * p, N8), n // N16)

    def c0(self, c):
        return self.send(self.cb.at[c, self.half(1 - self.core)], self.pbuf.at[c], self.p0s.at[c], self.p0r.at[c], self.mate)

    def c1(self, c, k, d):
        n = COLOR_ROWS[k] // N4
        a = self.coord[k]
        return self.send(self.cb.at[c, self.rows(k, (a + d) % N4)], self.r1.at[c, k, a, pl.ds(0, n)], self.p1s.at[c, k, d], self.p1r.at[c, k, d], self.peer(k, d))

    def c2(self, c, k, d):
        n = COLOR_ROWS[k] // N16
        b = (k + 1) % 3
        a = self.coord[b]
        src = self.cb.at[c, self.rows(k, self.coord[k], (a + d) % N4)]
        return self.send(src, self.r2.at[c, k, a, pl.ds(0, n)], self.p2s.at[c, k, d], self.p2r.at[c, k, d], self.peer(b, d))

    def c3(self, c, k, d):
        n = COLOR_ROWS[k] // N16
        b = (k + 2) % 3
        a = self.coord[b]
        src = self.cb.at[c, self.rows(k, self.coord[k], self.coord[(k + 1) % 3])]
        return self.send(src, self.r3.at[c, k, a, pl.ds(0, n)], self.p3s.at[c, k, d], self.p3r.at[c, k, d], self.peer(b, d))

    def c4(self, c, k, d):
        b = (k + 1) % 3
        part = self.res.at[c, self.rows(k, self.coord[k], self.coord[b])]
        return self.send(part, part, self.p4s.at[c, k, d], self.p4r.at[c, k, d], self.peer(b, d))

    def c5(self, c, k, d):
        part = self.res.at[c, self.rows(k, self.coord[k])]
        return self.send(part, part, self.p5s.at[c, k, d], self.p5r.at[c, k, d], self.peer(k, d))

    def c6(self, c):
        part = self.res.at[c, self.half(self.core)]
        return self.send(part, part, self.p6s.at[c], self.p6r.at[c], self.mate)

    def each(self, make, c):
        return [make(c, k, d) for d in (1, 3, 2) for k in range(3)]

    def phase(self, i, c):
        core = self.core
        if i == 0:
            self.c0(c).start()
        elif i == 1:
            self.c0(c).wait_recv()
            mine = self.half(core)
            self.cb[c, mine, :] = self.cb[c, mine, :] + self.pbuf[c]
            for x in self.each(self.c1, c):
                x.start()
        elif i == 2:
            for k in range(3):
                for d in (1, 3, 2):
                    self.c1(c, k, d).wait_recv()
                self.total(c, k, self.r1, self.rows(k, self.coord[k]), self.coord[k], COLOR_ROWS[k] // N4, self.cb)
                for d in (1, 3, 2):
                    self.c2(c, k, d).start()
        elif i == 3:
            for k in range(3):
                for d in (1, 3, 2):
                    self.c2(c, k, d).wait_recv()
                b = (k + 1) % 3
                self.total(c, k, self.r2, self.rows(k, self.coord[k], self.coord[b]), self.coord[b], COLOR_ROWS[k] // N16, self.cb)
                for d in (1, 3, 2):
                    self.c3(c, k, d).start()
        elif i == N4:
            for k in range(3):
                for d in (1, 3, 2):
                    self.c3(c, k, d).wait_recv()
                b = (k + 2) % 3
                self.total(c, k, self.r3, self.rows(k, self.coord[k], self.coord[(k + 1) % 3]), self.coord[b], COLOR_ROWS[k] // N16, self.res)
                for d in (1, 3, 2):
                    self.c4(c, k, d).start()
        elif i == 5:
            for k in range(3):
                for d in (1, 3, 2):
                    self.c4(c, k, d).wait_recv()
                for d in (1, 3, 2):
                    self.c5(c, k, d).start()
        elif i == 6:
            for k in range(3):
                for d in (1, 3, 2):
                    self.c5(c, k, d).wait_recv()
            self.c6(c).start()
        elif i == 7:
            self.c6(c).wait_recv()

    def total(self, c, k, slots, rows, a, n, out):
        slots[c, k, a, 0:n, :] = self.cb[c, rows, :]
        out[c, rows, :] = (slots[c, k, 0, 0:n, :] + slots[c, k, 1, 0:n, :]) + (slots[c, k, 2, 0:n, :] + slots[c, k, 3, 0:n, :])

    def finish(self, c):
        self.c0(c).wait_send()
        for make in (self.c1, self.c2, self.c3, self.c4, self.c5):
            for x in self.each(make, c):
                x.wait_send()
        self.c6(c).wait_send()


def reducer_scratch():
    sem = pltpu.SemaphoreType.DMA
    bufs = [pltpu.VMEM((N4, 2048, N128), F32), pltpu.VMEM((N4, N1024, N128), F32), pltpu.VMEM((N4, 3, N4, 96, N128), F32),
            pltpu.VMEM((N4, 3, N4, 24, N128), F32), pltpu.VMEM((N4, 3, N4, 24, N128), F32)]
    sems = [sem((N4,)), sem((N4,))] + [sem((N4, 3, N4))] * 10 + [sem((N4,)), sem((N4,))]
    return bufs, sems


def write_out(res, outs, sem, t):
    copies = []
    cols = pl.ds(pl.multiple_of(N128 * t, N128), N128)
    for i in range(3):
        copies.append(pltpu.make_async_copy(res.at[t, pl.ds(N512 * i, N512)], outs[i].at[:, cols], sem.at[t, i]))
    for j in range(N4):
        copies.append(pltpu.make_async_copy(res.at[t, pl.ds(1536 + N128 * j, N128)], outs[3].at[cols, pl.ds(N128 * j, N128)], sem.at[t, 3 + j]))
    return copies


def attention_kernel(x_ref, wq_ref, wk_ref, wv_ref, wo_ref, dy_ref, y_hbm, dx_hbm, o0, o1, o2, o3,
                     xp, dyp, qm, kt, vt, dom, g2, g3, keep, mh, lh, oh, lseh, delh, dqh, dka, dva, attnb, grads,
                     st2, st3, colt, rowt, s2s, s2r, s3s, s3r, t2s, t2r, t3s, t3r, y_buf, dx_buf, cb, res, pbuf, r1, r2, r3, wsem, osem, *rsems):
    red = Reducer(cb, res, pbuf, r1, r2, r3, rsems)
    me = red.me
    member = me % N4
    base = me - member
    peers = [None, red.mate, base + (member + 2 - N4 * (member // 2)), base + 3 - member]
    everyone = [peers[1], peers[3]] + [red.peer(ax, d) for ax in range(3) for d in (1, 2, 3)]

    barrier = pltpu.get_barrier_semaphore()
    for p in everyone:
        pl.semaphore_signal(barrier, inc=1, device_id={"sp": p}, device_id_type=MESH)

    ri = lax.broadcasted_iota(jnp.int32, (N256, N256), 0)
    ci = lax.broadcasted_iota(jnp.int32, (N256, N256), 1)
    blk = ri >> 5
    token = ((ri & 31) << 3) + ((blk & 1) << 2) + (blk & 2) + (blk >> 2)
    one = jnp.ones((), F32)
    zero = jnp.zeros((), F32)
    perm = jnp.where(token == ci, one, zero).astype(BF16)
    low = lanes_low(N512)
    keep[0] = jnp.where(low, one, zero).astype(BF16)
    keep[1] = jnp.where(low, zero, one).astype(BF16)

    def off2(t, par):
        return pl.multiple_of(N128 * par + N64 * (t % 2), N64)

    def off3(t, par):
        return pl.multiple_of(N128 * par + N64 * (t % 2) + N32 * (t // 2), N32)

    def lanes_of(i, n):
        return pl.ds(pl.multiple_of(i * n, n), n)

    def rows_of(s):
        return pl.ds(pl.multiple_of(N256 * s, N256), N256)

    for s in range(2):
        rows = slice(N256 * s, N256 * s + N256)
        xp[rows, :] = dot(perm, x_ref[rows, :]).astype(BF16)

    def project_kv(half, carry):
        cols = lanes_of(half, N256)
        for w, out in ((wk_ref, kt), (wv_ref, vt)):
            val = dot(xp[...], w[:, cols]).astype(BF16)
            out[2 * half] = val[:, :N128]
            out[2 * half + 1] = val[:, N128:]
        return carry

    def pack(a, ev, od, t):
        for g, n, off in ((g2, N64, N64 * (t % 2)), (g3, N32, N64 * (t % 2) + N32 * (t // 2))):
            for s in range(2):
                r = pl.multiple_of(N256 * s + off, N32)
                g[a, t, n * s:n * s + n, :] = ev(pl.ds(r, n)) * keep[0, :n, :] + od(pl.ds(r + N128, n)) * keep[1, :n, :]

    def pack_kv(t, carry):
        for a, ref in enumerate((kt, vt)):
            pack(a, lambda r: ref[t, r, :], lambda r: ref[t, r, :], t)
        return carry

    lax.fori_loop(0, 2, project_kv, 0)
    lax.fori_loop(0, N4, pack_kv, 0)

    def to2(a):
        return red.send(g2.at[a, :, pl.ds(0, N128), :], g2.at[a, :, pl.ds(N128, N128), :], s2s.at[a], s2r.at[a], peers[1])

    def to3(a, d):
        return red.send(g3.at[a, :, pl.ds(0, N64), :], g3.at[a, :, pl.ds(N64 * d, N64), :], s3s.at[a, d], s3r.at[a, d], peers[d])

    def send_group(arrays):
        for a in arrays:
            for d in (2, 3, 1):
                to3(a, d).start()
            to2(a).start()

    pl.semaphore_wait(barrier, len(everyone))
    send_group((0, 1))

    for s in range(2):
        rows = slice(N256 * s, N256 * s + N256)
        dyp[rows, :] = dot(perm, dy_ref[rows, :]).astype(BF16)

    def project_qo(half, carry):
        cols = lanes_of(half, N256)
        q = dot(xp[...], wq_ref[:, cols]).astype(BF16) * jnp.asarray(HEAD_DIM ** -0.5, BF16)
        d = dot(dyp[...], wo_ref[cols, :], NT).astype(BF16)
        for u in range(2):
            for par in range(2):
                qm[par, 2 * half + u] = q[:, N128 * u:N128 * u + N128] * keep[par]
                dom[par, 2 * half + u] = d[:, N128 * u:N128 * u + N128] * keep[par]
        return carry

    def pack_qo(t, carry):
        for a, ref in ((2, qm), (3, dom)):
            pack(a, lambda r: ref[0, t, r, :], lambda r: ref[1, t, r, :], t)
        return carry

    lax.fori_loop(0, 2, project_qo, 0)
    lax.fori_loop(0, N4, pack_qo, 0)
    send_group((2, 3))

    def forward(q, k, v):
        s = dot(q, k, NT)
        m = jnp.max(s, axis=1, keepdims=True)
        e = jnp.exp(s - m)
        l = jnp.sum(e, axis=1, keepdims=True)
        o = dot(e.astype(BF16), v)
        n = q.shape[0]
        return jnp.broadcast_to(m, (n, N128)), jnp.broadcast_to(l, (n, N128)), o

    def merge(h, start, n, m, l, o):
        m0 = two(mh, (h,), start, n)
        l0 = two(lh, (h,), start, n)
        o0 = two(oh, (h,), start, n)
        mn = jnp.maximum(m0, m)
        a = jnp.exp(m0 - mn)
        b = jnp.exp(m - mn)
        put_two(mh, (h,), start, n, mn)
        put_two(lh, (h,), start, n, l0 * a + l * b)
        put_two(oh, (h,), start, n, o0 * a + o * b)

    def fwd_local(h, carry):
        t, par = h // 2, h % 2
        for s in range(2):
            rows = slice(N256 * s, N256 * s + N256)
            m, l, o = forward(qm[par, t, rows, :], kt[t, rows, :], vt[t, rows, :])
            mh[h, rows, :] = m
            lh[h, rows, :] = l
            oh[h, rows, :] = o
        a = pl.multiple_of(N128 * par, N128)
        merge(h, a, N128, *forward(two(qm, (par, t), a, N128), two(kt, (t,), a, N128), two(vt, (t,), a, N128)))
        return carry

    lax.fori_loop(0, N8, fwd_local, 0)

    def fwd_mate(h, carry):
        t, par = h // 2, h % 2
        o2 = off2(t, par)
        merge(h, o2, N64, *forward(two(qm, (par, t), o2, N64), g2[0, t], g2[1, t]))
        return carry

    for a in range(2):
        to2(a).wait_recv()
    lax.fori_loop(0, N8, fwd_mate, 0)

    colt[...] = jnp.zeros_like(colt)

    def fwd_group(h, carry):
        t, par = h // 2, h % 2
        o3 = off3(t, par)
        merge(h, o3, N32, *forward(two(qm, (par, t), o3, N32), g3[0, t], g3[1, t]))
        lt = lh[h]
        att = oh[h] / lt
        lse = mh[h] + jnp.log(lt)
        delta = jnp.broadcast_to(jnp.sum(dom[par, t].astype(F32) * att, axis=1, keepdims=True), (N512, N128))
        oh[h] = att
        lseh[h] = lse
        delh[h] = delta
        lane = lax.broadcasted_iota(jnp.int32, (N512, N128), 1)
        colt[0:N512, :] = jnp.where(lane == h, lse, jnp.where(lane == h + N8, delta, colt[0:N512, :]))
        o2 = off2(t, par)
        lane = lane[:N128]
        colt[N512:N640, :] = jnp.where(lane == h, two(lseh, (h,), o2, N64), jnp.where(lane == h + N8, two(delh, (h,), o2, N64), colt[N512:N640, :]))
        l3 = two(lseh, (h,), o3, N32)
        d3 = two(delh, (h,), o3, N32)
        l3 = jnp.concatenate([l3, l3], axis=0)
        d3 = jnp.concatenate([d3, d3], axis=0)
        colt[N640:N768, :] = jnp.where(lane == h, l3, jnp.where(lane == h + N8, d3, colt[N640:N768, :]))
        return carry

    for a in range(2):
        for d in (1, 2, 3):
            to3(a, d).wait_recv()
    lax.fori_loop(0, N8, fwd_group, 0)

    st2[0] = jnp.transpose(colt[N512:N640, :])[:N16]
    st3[0] = jnp.transpose(colt[N640:N768, :])[:N16]

    def stat2():
        return red.send(st2.at[0], st2.at[1], t2s, t2r, peers[1])

    def stat3(d):
        return red.send(st3.at[0], st3.at[d], t3s.at[d], t3r.at[d], peers[d])

    for j in range(N4):
        rowt[j] = jnp.transpose(colt[N128 * j:N128 * j + N128, :])[:N16]
    for d in (2, 3):
        stat3(d).start()
    stat2().start()
    stat3(1).start()
    for t in range(N4):
        attnb[:, N128 * t:N128 * t + N128] = jnp.where(low, oh[2 * t], oh[2 * t + 1]).astype(BF16)

    def transposed_grads(q, d_rows, k, v, lse_row, delta_row):
        pt = jnp.exp(dot(k, q, NT) - lse_row)
        dst = (pt * (dot(v, d_rows, NT) - delta_row)).astype(BF16)
        return dot(dst, q), dot(pt.astype(BF16), d_rows), dst

    def grad_q(q, d_rows, k, v, lse, delta):
        p = jnp.exp(dot(q, k, NT) - wide(lse))
        ds = (p * (dot(d_rows, v, NT) - wide(delta))).astype(BF16)
        return dot(ds, k)

    lo1 = lax.broadcasted_iota(jnp.int32, (1, N128), 1) < N64

    def wait_stats():
        stat2().wait_recv()
        for d in (1, 2, 3):
            stat3(d).wait_recv()
        for a in (2, 3):
            to2(a).wait_recv()
            for d in (1, 2, 3):
                to3(a, d).wait_recv()

    def rows2(i, j, h):
        return jnp.concatenate([rowt[i, pl.ds(h, 1), :], rowt[j, pl.ds(h, 1), :]], axis=1)

    def backward(t, par):
        h = 2 * t + par

        @pl.when(par == 0)
        def _():
            dka[...] = jnp.zeros_like(dka)
            dva[...] = jnp.zeros_like(dva)

        for s in range(2):
            rows = slice(N256 * s, N256 * s + N256)
            k = kt[t, rows, :]
            gk, gv, dst = transposed_grads(qm[par, t, rows, :], dom[par, t, rows, :], k, vt[t, rows, :], rows2(2 * s, 2 * s + 1, h), rows2(2 * s, 2 * s + 1, h + N8))
            dqh[par, rows, :] = dot(dst, k, TN)
            dka[rows, :] += gk
            dva[rows, :] += gv
        a = pl.multiple_of(N128 * par, N128)
        lr, dr = rows2(par, 2 + par, h), rows2(par, 2 + par, h + N8)
        k = two(kt, (t,), a, N128)
        gk, gv, dst = transposed_grads(two(qm, (par, t), a, N128), two(dom, (par, t), a, N128), k, two(vt, (t,), a, N128), lr, dr)
        add_two(dqh, (par,), a, N128, dot(dst, k, TN))
        add_two(dka, (), a, N128, gk)
        add_two(dva, (), a, N128, gv)

        pl.when(h == 0)(wait_stats)
        off = off2(t, par)
        q, d_rows = two(qm, (par, t), off, N64), two(dom, (par, t), off, N64)
        add_two(dqh, (par,), off, N64, grad_q(q, d_rows, g2[0, t], g2[1, t], two(lseh, (h,), off, N64), two(delh, (h,), off, N64)))
        lr = jnp.concatenate([st2[0, pl.ds(h, 1), :], st2[1, pl.ds(h, 1), :]], axis=1)
        dr = jnp.concatenate([st2[0, pl.ds(h + N8, 1), :], st2[1, pl.ds(h + N8, 1), :]], axis=1)
        gk, gv, _ = transposed_grads(g2[2, t] * keep[par, :N256, :], g2[3, t] * keep[par, :N256, :], two(kt, (t,), off, N64), two(vt, (t,), off, N64), lr, dr)
        add_two(dka, (), off, N64, gk)
        add_two(dva, (), off, N64, gv)
        off = off3(t, par)
        q, d_rows = two(qm, (par, t), off, N32), two(dom, (par, t), off, N32)
        add_two(dqh, (par,), off, N32, grad_q(q, d_rows, g3[0, t], g3[1, t], two(lseh, (h,), off, N32), two(delh, (h,), off, N32)))

        def row3(i):
            r = [st3[d, pl.ds(i, 1), :] for d in range(N4)]
            return jnp.concatenate([jnp.where(lo1, r[0], r[1]), jnp.where(lo1, r[2], r[3])], axis=1)

        gk, gv, _ = transposed_grads(g3[2, t] * keep[par, :N256, :], g3[3, t] * keep[par, :N256, :], two(kt, (t,), off, N32), two(vt, (t,), off, N32), row3(h), row3(h + N8))
        add_two(dka, (), off, N32, gk)
        add_two(dva, (), off, N32, gv)

    def chunk(t):
        cols = lanes_of(t, N128)
        dq = jnp.where(low, dqh[0], dqh[1]) * (HEAD_DIM ** -0.5)
        for i, g in enumerate((dq, dka[...], dva[...])):
            gb = g.astype(BF16)
            grads[i, :, cols] = gb
            cb[t, N512 * i:N512 * i + N512, :] = dot(xp[...], gb, TN)
        g = dot(attnb[:, cols], dyp[...], TN)
        for j in range(N4):
            cb[t, 1536 + N128 * j:1664 + N128 * j, :] = g[:, N128 * j:N128 * j + N128]

    def pair(t, carry):
        def head(par, c):
            backward(t, par)
            return c

        lax.fori_loop(0, 2, head, 0)
        chunk(t)
        red.phase(0, t)
        for i in range(1, N4):
            @pl.when(t >= i)
            def _():
                red.phase(i, t - i)
        return carry

    lax.fori_loop(0, N4, pair, 0)

    def y_part(s):
        rows = slice(N256 * s, N256 * s + N256)
        yb = dot(attnb[rows, :], wo_ref[...]).astype(BF16)
        y_buf[rows, :] = dot(perm, yb, TN).astype(BF16)

    def dx_part(s):
        rows = slice(N256 * s, N256 * s + N256)
        dxb = (dot(grads[0, rows, :], wq_ref[...], NT) + dot(grads[1, rows, :], wk_ref[...], NT) + dot(grads[2, rows, :], wv_ref[...], NT)).astype(BF16)
        dx_buf[rows, :] = dot(perm, dxb, TN).astype(BF16)

    def done(c):
        red.phase(7, c)
        for x in write_out(res, (o0, o1, o2, o3), wsem, c):
            x.start()

    y_out = pltpu.make_async_copy(y_buf, y_hbm, osem.at[0])
    dx_out = pltpu.make_async_copy(dx_buf, dx_hbm, osem.at[1])
    red.phase(1, 3)
    red.phase(2, 2)
    red.phase(3, 1)
    red.phase(N4, 0)
    dx_part(0)
    red.phase(2, 3)
    red.phase(3, 2)
    red.phase(N4, 1)
    red.phase(5, 0)
    dx_part(1)
    red.phase(3, 3)
    red.phase(N4, 2)
    red.phase(5, 1)
    y_part(0)
    red.phase(N4, 3)
    red.phase(5, 2)
    red.phase(6, 0)
    y_part(1)
    red.phase(5, 3)
    y_out.start()
    dx_out.start()
    done(0)
    red.phase(6, 1)
    red.phase(6, 2)
    done(1)
    red.phase(6, 3)
    done(2)
    done(3)

    for a in range(N4):
        to2(a).wait_send()
        for d in (1, 2, 3):
            to3(a, d).wait_send()
    stat2().wait_send()
    for d in (1, 2, 3):
        stat3(d).wait_send()

    def finish(c, carry):
        red.finish(c)
        for x in write_out(res, (o0, o1, o2, o3), wsem, c):
            x.wait()
        return carry

    lax.fori_loop(0, N4, finish, 0)
    y_out.wait()
    dx_out.wait()


def attention(x_loc, w_q, w_k, w_v, w_o, dy_loc):
    vmem = pl.BlockSpec(memory_space=pltpu.VMEM)
    sem = pltpu.SemaphoreType.DMA
    bufs, sems = reducer_scratch()
    act = pltpu.VMEM((N512, N512), BF16)
    pairs = pltpu.VMEM((N4, N512, N128), BF16)
    heads = pltpu.VMEM((N8, N512, N128), F32)
    return pl.pallas_call(
        attention_kernel,
        out_shape=[jax.ShapeDtypeStruct((N512, N512), BF16)] * 2 + [jax.ShapeDtypeStruct((N512, N512), F32)] * N4,
        in_specs=[vmem] * 6,
        out_specs=[pl.BlockSpec(memory_space=pl.ANY)] * 6,
        scratch_shapes=[
            act, act, pltpu.VMEM((2, N4, N512, N128), BF16), pairs, pairs, pltpu.VMEM((2, N4, N512, N128), BF16),
            pltpu.VMEM((N4, N4, N256, N128), BF16), pltpu.VMEM((N4, N4, N256, N128), BF16), pltpu.VMEM((2, N512, N128), BF16),
            heads, heads, heads, heads, heads,
            pltpu.VMEM((2, N512, N128), F32), pltpu.VMEM((N512, N128), F32), pltpu.VMEM((N512, N128), F32), act, pltpu.VMEM((3, N512, N512), BF16),
            pltpu.VMEM((2, N16, N128), F32), pltpu.VMEM((N4, N16, N128), F32), pltpu.VMEM((N768, N128), F32), pltpu.VMEM((N4, N16, N128), F32),
            sem((N4,)), sem((N4,)), sem((N4, N4)), sem((N4, N4)), sem, sem, sem((N4,)), sem((N4,)),
            act, act, pltpu.VMEM((N4, 2048, N128), F32),
        ] + bufs + [sem((N4, 7)), sem((2,))] + sems,
        compiler_params=pltpu.CompilerParams(collective_id=0, has_side_effects=True, vmem_limit_bytes=60 * 2 ** 20),
        name="attention_step",
    )(x_loc, w_q, w_k, w_v, w_o, dy_loc)


def solution(mesh):
    def device_step(x_loc, w_q, w_k, w_v, w_o, dy_loc):
        return tuple(attention(x_loc, w_q, w_k, w_v, w_o, dy_loc))

    row_spec = P(("dp", "sp"), None)
    full_spec = P(None, None)
    grad_spec = P("dp", None)
    return jax.shard_map(device_step, mesh=mesh, in_specs=(row_spec, full_spec, full_spec, full_spec, full_spec, row_spec),
                         out_specs=(row_spec, row_spec, grad_spec, grad_spec, grad_spec, grad_spec), check_vma=False)
```

```python
import functools

import jax
import jax.numpy as jnp
from jax import lax
from jax.experimental import pallas as pl
from jax.experimental.pallas import tpu as pltpu
from jax.sharding import PartitionSpec as P

HEAD_DIM = 64
N4 = 4
N8 = 8
N16 = 16
N32 = 32
N64 = 64
N128 = 128
N256 = 256
N512 = 512
N640 = 640
N768 = 768
N1024 = 1024
F32 = jnp.float32
BF16 = jnp.bfloat16
MESH = pl.DeviceIdType.MESH
NN = (((1,), (0,)), ((), ()))
NT = (((1,), (1,)), ((), ()))
TN = (((0,), (0,)), ((), ()))


def dot(a, b, dims=NN):
    return lax.dot_general(a, b, dims, preferred_element_type=F32)


def two(ref, lead, start, n):
    return jnp.concatenate([ref[lead + (pl.ds(start, n), slice(None))], ref[lead + (pl.ds(N256 + start, n), slice(None))]], axis=0)


def put_two(ref, lead, start, n, val):
    ref[lead + (pl.ds(start, n), slice(None))] = val[:n]
    ref[lead + (pl.ds(N256 + start, n), slice(None))] = val[n:]


def wide(stat):
    return jnp.concatenate([stat, stat], axis=1)


def add_two(ref, lead, start, n, val):
    put_two(ref, lead, start, n, two(ref, lead, start, n) + val)


def lanes_low(rows):
    return lax.broadcasted_iota(jnp.int32, (rows, N128), 1) < N64


COLOR_ROWS = (384, 384, N256)
COLOR_BASE = (0, 384, N768)
STRIDES = (2, N8, N32)


class Reducer:
    def __init__(self, cb, res, pbuf, r1, r2, r3, sems):
        self.cb, self.res, self.pbuf, self.r1, self.r2, self.r3 = cb, res, pbuf, r1, r2, r3
        (self.p0s, self.p0r, self.p1s, self.p1r, self.p2s, self.p2r, self.p3s, self.p3r,
         self.p4s, self.p4r, self.p5s, self.p5r, self.p6s, self.p6r) = sems
        self.me = lax.axis_index("sp")
        self.core = self.me % 2
        self.coord = [(self.me // s) % N4 for s in STRIDES]
        self.mate = self.me + 1 - 2 * self.core

    def peer(self, axis, d):
        return self.me + STRIDES[axis] * ((self.coord[axis] + d) % N4 - self.coord[axis])

    def send(self, src, dst, ss, rs, dev):
        return pltpu.make_async_remote_copy(src_ref=src, dst_ref=dst, send_sem=ss, recv_sem=rs, device_id={"sp": dev}, device_id_type=MESH)

    def half(self, core):
        return pl.ds(pl.multiple_of(N1024 * core, N1024), N1024)

    def rows(self, k, q, p=None):
        n = COLOR_ROWS[k]
        start = N1024 * self.core + COLOR_BASE[k] + (n // N4) * q
        if p is None:
            return pl.ds(pl.multiple_of(start, N8), n // N4)
        return pl.ds(pl.multiple_of(start + (n // N16) * p, N8), n // N16)

    def c0(self, c):
        return self.send(self.cb.at[c, self.half(1 - self.core)], self.pbuf.at[c], self.p0s.at[c], self.p0r.at[c], self.mate)

    def c1(self, c, k, d):
        n = COLOR_ROWS[k] // N4
        a = self.coord[k]
        return self.send(self.cb.at[c, self.rows(k, (a + d) % N4)], self.r1.at[c, k, a, pl.ds(0, n)], self.p1s.at[c, k, d], self.p1r.at[c, k, d], self.peer(k, d))

    def c2(self, c, k, d):
        n = COLOR_ROWS[k] // N16
        b = (k + 1) % 3
        a = self.coord[b]
        src = self.cb.at[c, self.rows(k, self.coord[k], (a + d) % N4)]
        return self.send(src, self.r2.at[c, k, a, pl.ds(0, n)], self.p2s.at[c, k, d], self.p2r.at[c, k, d], self.peer(b, d))

    def c3(self, c, k, d):
        n = COLOR_ROWS[k] // N16
        b = (k + 2) % 3
        a = self.coord[b]
        src = self.cb.at[c, self.rows(k, self.coord[k], self.coord[(k + 1) % 3])]
        return self.send(src, self.r3.at[c, k, a, pl.ds(0, n)], self.p3s.at[c, k, d], self.p3r.at[c, k, d], self.peer(b, d))

    def c4(self, c, k, d):
        b = (k + 1) % 3
        part = self.res.at[c, self.rows(k, self.coord[k], self.coord[b])]
        return self.send(part, part, self.p4s.at[c, k, d], self.p4r.at[c, k, d], self.peer(b, d))

    def c5(self, c, k, d):
        part = self.res.at[c, self.rows(k, self.coord[k])]
        return self.send(part, part, self.p5s.at[c, k, d], self.p5r.at[c, k, d], self.peer(k, d))

    def c6(self, c):
        part = self.res.at[c, self.half(self.core)]
        return self.send(part, part, self.p6s.at[c], self.p6r.at[c], self.mate)

    def each(self, make, c):
        return [make(c, k, d) for d in (1, 3, 2) for k in range(3)]

    def phase(self, i, c):
        core = self.core
        if i == 0:
            self.c0(c).start()
        elif i == 1:
            self.c0(c).wait_recv()
            mine = self.half(core)
            self.cb[c, mine, :] = self.cb[c, mine, :] + self.pbuf[c]
            for x in self.each(self.c1, c):
                x.start()
        elif i == 2:
            for k in range(3):
                for d in (1, 3, 2):
                    self.c1(c, k, d).wait_recv()
                self.total(c, k, self.r1, self.rows(k, self.coord[k]), self.coord[k], COLOR_ROWS[k] // N4, self.cb)
                for d in (1, 3, 2):
                    self.c2(c, k, d).start()
        elif i == 3:
            for k in range(3):
                for d in (1, 3, 2):
                    self.c2(c, k, d).wait_recv()
                b = (k + 1) % 3
                self.total(c, k, self.r2, self.rows(k, self.coord[k], self.coord[b]), self.coord[b], COLOR_ROWS[k] // N16, self.cb)
                for d in (1, 3, 2):
                    self.c3(c, k, d).start()
        elif i == N4:
            for k in range(3):
                for d in (1, 3, 2):
                    self.c3(c, k, d).wait_recv()
                b = (k + 2) % 3
                self.total(c, k, self.r3, self.rows(k, self.coord[k], self.coord[(k + 1) % 3]), self.coord[b], COLOR_ROWS[k] // N16, self.res)
                for d in (1, 3, 2):
                    self.c4(c, k, d).start()
        elif i == 5:
            for k in range(3):
                for d in (1, 3, 2):
                    self.c4(c, k, d).wait_recv()
                for d in (1, 3, 2):
                    self.c5(c, k, d).start()
        elif i == 6:
            for k in range(3):
                for d in (1, 3, 2):
                    self.c5(c, k, d).wait_recv()
            self.c6(c).start()
        elif i == 7:
            self.c6(c).wait_recv()

    def total(self, c, k, slots, rows, a, n, out):
        slots[c, k, a, 0:n, :] = self.cb[c, rows, :]
        out[c, rows, :] = (slots[c, k, 0, 0:n, :] + slots[c, k, 1, 0:n, :]) + (slots[c, k, 2, 0:n, :] + slots[c, k, 3, 0:n, :])

    def finish(self, c):
        self.c0(c).wait_send()
        for make in (self.c1, self.c2, self.c3, self.c4, self.c5):
            for x in self.each(make, c):
                x.wait_send()
        self.c6(c).wait_send()


def reducer_scratch():
    sem = pltpu.SemaphoreType.DMA
    bufs = [pltpu.VMEM((N4, 2048, N128), F32), pltpu.VMEM((N4, N1024, N128), F32), pltpu.VMEM((N4, 3, N4, 96, N128), F32),
            pltpu.VMEM((N4, 3, N4, 24, N128), F32), pltpu.VMEM((N4, 3, N4, 24, N128), F32)]
    sems = [sem((N4,)), sem((N4,))] + [sem((N4, 3, N4))] * 10 + [sem((N4,)), sem((N4,))]
    return bufs, sems


def write_out(res, outs, sem, t):
    copies = []
    cols = pl.ds(pl.multiple_of(N128 * t, N128), N128)
    for i in range(3):
        copies.append(pltpu.make_async_copy(res.at[t, pl.ds(N512 * i, N512)], outs[i].at[:, cols], sem.at[t, i]))
    for j in range(N4):
        copies.append(pltpu.make_async_copy(res.at[t, pl.ds(1536 + N128 * j, N128)], outs[3].at[cols, pl.ds(N128 * j, N128)], sem.at[t, 3 + j]))
    return copies


def attention_kernel(x_hbm, wq_hbm, wk_hbm, wv_hbm, wo_hbm, dy_hbm, y_buf, dx_buf, res,
                     x_ref, wq_ref, wk_ref, wv_ref, wo_ref, dy_ref, isem, xp, dyp, qm, kt, vt, dom, g2, g3, keep, mh, lh, oh, lseh, delh, dqh, dka, dva, attnb, grads,
                     st2, st3, colt, rowt, s2s, s2r, s3s, s3r, t2s, t2r, t3s, t3r, cb, pbuf, r1, r2, r3, *rsems):
    red = Reducer(cb, res, pbuf, r1, r2, r3, rsems)
    me = red.me
    member = me % N4
    base = me - member
    peers = [None, red.mate, base + (member + 2 - N4 * (member // 2)), base + 3 - member]
    everyone = [peers[1], peers[3]] + [red.peer(ax, d) for ax in range(3) for d in (1, 2, 3)]

    barrier = pltpu.get_barrier_semaphore()
    for p in everyone:
        pl.semaphore_signal(barrier, inc=1, device_id={"sp": p}, device_id_type=MESH)

    loads = [pltpu.make_async_copy(src, dst, isem.at[i]) for i, (src, dst) in enumerate(
        ((x_hbm, x_ref), (wk_hbm, wk_ref), (wv_hbm, wv_ref), (dy_hbm, dy_ref), (wq_hbm, wq_ref), (wo_hbm, wo_ref)))]
    for x in loads:
        x.start()

    ri = lax.broadcasted_iota(jnp.int32, (N256, N256), 0)
    ci = lax.broadcasted_iota(jnp.int32, (N256, N256), 1)
    blk = ri >> 5
    token = ((ri & 31) << 3) + ((blk & 1) << 2) + (blk & 2) + (blk >> 2)
    one = jnp.ones((), F32)
    zero = jnp.zeros((), F32)
    perm = jnp.where(token == ci, one, zero).astype(BF16)
    low = lanes_low(N512)
    keep[0] = jnp.where(low, one, zero).astype(BF16)
    keep[1] = jnp.where(low, zero, one).astype(BF16)

    def off2(t, par):
        return pl.multiple_of(N128 * par + N64 * (t % 2), N64)

    def off3(t, par):
        return pl.multiple_of(N128 * par + N64 * (t % 2) + N32 * (t // 2), N32)

    def lanes_of(i, n):
        return pl.ds(pl.multiple_of(i * n, n), n)

    def rows_of(s):
        return pl.ds(pl.multiple_of(N256 * s, N256), N256)

    for x in loads[:3]:
        x.wait()
    for s in range(2):
        rows = slice(N256 * s, N256 * s + N256)
        xp[rows, :] = dot(perm, x_ref[rows, :]).astype(BF16)

    def project_kv(half, carry):
        cols = lanes_of(half, N256)
        for w, out in ((wk_ref, kt), (wv_ref, vt)):
            val = dot(xp[...], w[:, cols]).astype(BF16)
            out[2 * half] = val[:, :N128]
            out[2 * half + 1] = val[:, N128:]
        return carry

    def pack(a, ev, od, t):
        for g, n, off in ((g2, N64, N64 * (t % 2)), (g3, N32, N64 * (t % 2) + N32 * (t // 2))):
            for s in range(2):
                r = pl.multiple_of(N256 * s + off, N32)
                g[a, t, n * s:n * s + n, :] = ev(pl.ds(r, n)) * keep[0, :n, :] + od(pl.ds(r + N128, n)) * keep[1, :n, :]

    def pack_kv(t, carry):
        for a, ref in enumerate((kt, vt)):
            pack(a, lambda r: ref[t, r, :], lambda r: ref[t, r, :], t)
        return carry

    lax.fori_loop(0, 2, project_kv, 0)
    lax.fori_loop(0, N4, pack_kv, 0)

    def to2(a):
        return red.send(g2.at[a, :, pl.ds(0, N128), :], g2.at[a, :, pl.ds(N128, N128), :], s2s.at[a], s2r.at[a], peers[1])

    def to3(a, d):
        return red.send(g3.at[a, :, pl.ds(0, N64), :], g3.at[a, :, pl.ds(N64 * d, N64), :], s3s.at[a, d], s3r.at[a, d], peers[d])

    def send_group(arrays):
        for a in arrays:
            for d in (2, 3, 1):
                to3(a, d).start()
            to2(a).start()

    for x in loads[3:]:
        x.wait()
    for s in range(2):
        rows = slice(N256 * s, N256 * s + N256)
        dyp[rows, :] = dot(perm, dy_ref[rows, :]).astype(BF16)

    def project_qo(half, carry):
        cols = lanes_of(half, N256)
        q = dot(xp[...], wq_ref[:, cols]).astype(BF16) * jnp.asarray(HEAD_DIM ** -0.5, BF16)
        d = dot(dyp[...], wo_ref[cols, :], NT).astype(BF16)
        for u in range(2):
            for par in range(2):
                qm[par, 2 * half + u] = q[:, N128 * u:N128 * u + N128] * keep[par]
                dom[par, 2 * half + u] = d[:, N128 * u:N128 * u + N128] * keep[par]
        return carry

    def pack_qo(t, carry):
        for a, ref in ((2, qm), (3, dom)):
            pack(a, lambda r: ref[0, t, r, :], lambda r: ref[1, t, r, :], t)
        return carry

    lax.fori_loop(0, 2, project_qo, 0)
    lax.fori_loop(0, N4, pack_qo, 0)
    pl.semaphore_wait(barrier, len(everyone))
    send_group(range(N4))

    def forward(q, k, v):
        s = dot(q, k, NT)
        m = jnp.max(s, axis=1, keepdims=True)
        e = jnp.exp(s - m)
        l = jnp.sum(e, axis=1, keepdims=True)
        o = dot(e.astype(BF16), v)
        n = q.shape[0]
        return jnp.broadcast_to(m, (n, N128)), jnp.broadcast_to(l, (n, N128)), o

    def merge(h, start, n, m, l, o):
        m0 = two(mh, (h,), start, n)
        l0 = two(lh, (h,), start, n)
        o0 = two(oh, (h,), start, n)
        mn = jnp.maximum(m0, m)
        a = jnp.exp(m0 - mn)
        b = jnp.exp(m - mn)
        put_two(mh, (h,), start, n, mn)
        put_two(lh, (h,), start, n, l0 * a + l * b)
        put_two(oh, (h,), start, n, o0 * a + o * b)

    def fwd_local(t, carry):
        got = []
        for par in range(2):
            segs = [forward(qm[par, t, N256 * s:N256 * s + N256, :], kt[t, N256 * s:N256 * s + N256, :], vt[t, N256 * s:N256 * s + N256, :]) for s in range(2)]
            a = N128 * par
            got.append((segs, forward(two(qm, (par, t), a, N128), two(kt, (t,), a, N128), two(vt, (t,), a, N128))))
        for par in range(2):
            h = 2 * t + par
            segs, both = got[par]
            for s in range(2):
                a = N128 * par
                m, l, o = segs[s]
                mb, lb, ob = [v[N128 * s:N128 * s + N128] for v in both]
                ma, la, oa = [v[a:a + N128] for v in segs[s]]
                mn = jnp.maximum(ma, mb)
                wa = jnp.exp(ma - mn)
                wb = jnp.exp(mb - mn)
                r = N256 * s + a
                z = N256 * s + N128 - a
                mh[h, r:r + N128, :] = mn
                lh[h, r:r + N128, :] = la * wa + lb * wb
                oh[h, r:r + N128, :] = oa * wa + ob * wb
                mh[h, z:z + N128, :] = m[N128 - a:N256 - a]
                lh[h, z:z + N128, :] = l[N128 - a:N256 - a]
                oh[h, z:z + N128, :] = o[N128 - a:N256 - a]
        return carry

    lax.fori_loop(0, N4, fwd_local, 0)

    def fwd_mate(t, carry):
        got = [forward(two(qm, (par, t), off2(t, par), N64), g2[0, t], g2[1, t]) for par in range(2)]
        for par in range(2):
            merge(2 * t + par, off2(t, par), N64, *got[par])
        return carry

    for a in range(2):
        to2(a).wait_recv()
    lax.fori_loop(0, N4, fwd_mate, 0)

    colt[...] = jnp.zeros_like(colt)

    def fwd_group(t, carry):
        got = [forward(two(qm, (par, t), off3(t, par), N32), g3[0, t], g3[1, t]) for par in range(2)]
        for par in range(2):
            merge(2 * t + par, off3(t, par), N32, *got[par])
        atts, stats = [], []
        for par in range(2):
            h = 2 * t + par
            lt = lh[h]
            att = oh[h] / lt
            lse = mh[h] + jnp.log(lt)
            delta = jnp.broadcast_to(jnp.sum(dom[par, t].astype(F32) * att, axis=1, keepdims=True), (N512, N128))
            atts.append(att)
            stats.append((lse, delta))
            lseh[h] = lse
            delh[h] = delta
        attnb[:, lanes_of(t, N128)] = jnp.where(low, atts[0], atts[1]).astype(BF16)

        def columns(part, n, take):
            lane = lax.broadcasted_iota(jnp.int32, (n, N128), 1)
            val = colt[part, :]
            for par in range(2):
                h = 2 * t + par
                lse, delta = take(par, h)
                val = jnp.where(lane == h, lse, jnp.where(lane == h + N8, delta, val))
            colt[part, :] = val

        def twice(v):
            return jnp.concatenate([v, v], axis=0)

        columns(slice(0, N512), N512, lambda par, h: stats[par])
        columns(slice(N512, N640), N128, lambda par, h: [two(r, (h,), off2(t, par), N64) for r in (lseh, delh)])
        columns(slice(N640, N768), N128, lambda par, h: [twice(two(r, (h,), off3(t, par), N32)) for r in (lseh, delh)])
        return carry

    for a in range(2):
        for d in (1, 2, 3):
            to3(a, d).wait_recv()
    lax.fori_loop(0, N4, fwd_group, 0)

    st2[0] = jnp.transpose(colt[N512:N640, :])[:N16]
    st3[0] = jnp.transpose(colt[N640:N768, :])[:N16]

    def stat2():
        return red.send(st2.at[0], st2.at[1], t2s, t2r, peers[1])

    def stat3(d):
        return red.send(st3.at[0], st3.at[d], t3s.at[d], t3r.at[d], peers[d])

    for j in range(N4):
        rowt[j] = jnp.transpose(colt[N128 * j:N128 * j + N128, :])[:N16]
    for d in (2, 3):
        stat3(d).start()
    stat2().start()
    stat3(1).start()

    def transposed_grads(q, d_rows, k, v, lse_row, delta_row):
        pt = jnp.exp(dot(k, q, NT) - lse_row)
        dst = (pt * (dot(v, d_rows, NT) - delta_row)).astype(BF16)
        return dot(dst, q), dot(pt.astype(BF16), d_rows), dst

    def grad_q(q, d_rows, k, v, lse, delta):
        p = jnp.exp(dot(q, k, NT) - wide(lse))
        ds = (p * (dot(d_rows, v, NT) - wide(delta))).astype(BF16)
        return dot(ds, k)

    lo1 = lax.broadcasted_iota(jnp.int32, (1, N128), 1) < N64

    def wait_stats():
        stat2().wait_recv()
        for d in (1, 2, 3):
            stat3(d).wait_recv()
        for a in (2, 3):
            to2(a).wait_recv()
            for d in (1, 2, 3):
                to3(a, d).wait_recv()

    def rows2(i, j, h):
        return jnp.concatenate([rowt[i, pl.ds(h, 1), :], rowt[j, pl.ds(h, 1), :]], axis=1)

    def backward_local(t):
        got = []
        for par in range(2):
            h = 2 * t + par
            tiles = []
            for s in range(3):
                if s < 2:
                    q, d_rows, k, v = [r[lead + (slice(N256 * s, N256 * s + N256), slice(0, N128))] for r, lead in ((qm, (par, t)), (dom, (par, t)), (kt, (t,)), (vt, (t,)))]
                    i, j = 2 * s, 2 * s + 1
                else:
                    q, d_rows, k, v = [two(r, lead, N128 * par, N128) for r, lead in ((qm, (par, t)), (dom, (par, t)), (kt, (t,)), (vt, (t,)))]
                    i, j = par, 2 + par
                gk, gv, dst = transposed_grads(q, d_rows, k, v, rows2(i, j, h), rows2(i, j, h + N8))
                tiles.append((dot(dst, k, TN), gk, gv))
            got.append(tiles)
        for par in range(2):
            a = N128 * par
            for s in range(2):
                for ref, own, both in zip((dqh, dka, dva), got[par][s], got[par][2]):
                    r = N256 * s + a
                    z = N256 * s + N128 - a
                    ref[par, r:r + N128, :] = own[a:a + N128] + both[N128 * s:N128 * s + N128]
                    ref[par, z:z + N128, :] = own[N128 - a:N256 - a]

    def row3(i):
        r = [st3[d, pl.ds(i, 1), :] for d in range(N4)]
        return jnp.concatenate([jnp.where(lo1, r[0], r[1]), jnp.where(lo1, r[2], r[3])], axis=1)

    def row2(i):
        return jnp.concatenate([st2[0, pl.ds(i, 1), :], st2[1, pl.ds(i, 1), :]], axis=1)

    def backward_group(t):
        got = []
        for g, n, off, row in ((g2, N64, off2, row2), (g3, N32, off3, row3)):
            for par in range(2):
                h = 2 * t + par
                r = off(t, par)
                gq = grad_q(two(qm, (par, t), r, n), two(dom, (par, t), r, n), g[0, t], g[1, t], two(lseh, (h,), r, n), two(delh, (h,), r, n))
                gk, gv, _ = transposed_grads(g[2, t] * keep[par, :N256, :], g[3, t] * keep[par, :N256, :], two(kt, (t,), r, n), two(vt, (t,), r, n), row(h), row(h + N8))
                got.append((par, r, n, (gq, gk, gv)))
        for par, r, n, vals in got:
            for ref, val in zip((dqh, dka, dva), vals):
                add_two(ref, (par,), r, n, val)

    def chunk(t):
        cols = lanes_of(t, N128)
        dq = jnp.where(low, dqh[0], dqh[1]) * (HEAD_DIM ** -0.5)
        for i, g in enumerate((dq, dka[0] + dka[1], dva[0] + dva[1])):
            gb = g.astype(BF16)
            grads[i, :, cols] = gb
            cb[t, N512 * i:N512 * i + N512, :] = dot(xp[...], gb, TN)
        g = dot(attnb[:, cols], dyp[...], TN)
        for j in range(N4):
            cb[t, 1536 + N128 * j:1664 + N128 * j, :] = g[:, N128 * j:N128 * j + N128]

    def pair(t, carry):
        backward_local(t)
        pl.when(t == 0)(wait_stats)
        backward_group(t)
        chunk(t)
        red.phase(0, t)
        for i in range(1, N4):
            @pl.when(t >= i)
            def _():
                red.phase(i, t - i)
        return carry

    lax.fori_loop(0, N4, pair, 0)

    def y_part(s):
        rows = slice(N256 * s, N256 * s + N256)
        yb = dot(attnb[rows, :], wo_ref[...]).astype(BF16)
        y_buf[rows, :] = dot(perm, yb, TN).astype(BF16)

    def dx_part(s):
        rows = slice(N256 * s, N256 * s + N256)
        dxb = (dot(grads[0, rows, :], wq_ref[...], NT) + dot(grads[1, rows, :], wk_ref[...], NT) + dot(grads[2, rows, :], wv_ref[...], NT)).astype(BF16)
        dx_buf[rows, :] = dot(perm, dxb, TN).astype(BF16)

    def done(c):
        red.phase(7, c)

    red.phase(1, 3)
    red.phase(2, 2)
    red.phase(3, 1)
    red.phase(N4, 0)
    dx_part(0)
    red.phase(2, 3)
    red.phase(3, 2)
    red.phase(N4, 1)
    red.phase(5, 0)
    dx_part(1)
    red.phase(3, 3)
    red.phase(N4, 2)
    red.phase(5, 1)
    y_part(0)
    red.phase(N4, 3)
    red.phase(5, 2)
    red.phase(6, 0)
    y_part(1)
    red.phase(5, 3)
    done(0)
    red.phase(6, 1)
    red.phase(6, 2)
    done(1)
    red.phase(6, 3)
    done(2)
    done(3)

    for a in range(N4):
        to2(a).wait_send()
        for d in (1, 2, 3):
            to3(a, d).wait_send()
    stat2().wait_send()
    for d in (1, 2, 3):
        stat3(d).wait_send()

    def finish(c, carry):
        red.finish(c)
        return carry

    lax.fori_loop(0, N4, finish, 0)


def write_kernel(y_buf, dx_buf, res, y_hbm, dx_hbm, o0, o1, o2, o3, wsem, osem):
    copies = [pltpu.make_async_copy(y_buf, y_hbm, osem.at[0]), pltpu.make_async_copy(dx_buf, dx_hbm, osem.at[1])]
    for t in range(N4):
        copies += write_out(res, (o0, o1, o2, o3), wsem, t)
    for x in copies:
        x.start()
    for x in copies:
        x.wait()


def attention(x_loc, w_q, w_k, w_v, w_o, dy_loc):
    vmem = pl.BlockSpec(memory_space=pltpu.VMEM)
    hbm = pl.BlockSpec(memory_space=pltpu.HBM)
    sem = pltpu.SemaphoreType.DMA
    bufs, sems = reducer_scratch()
    act = pltpu.VMEM((N512, N512), BF16)
    pairs = pltpu.VMEM((N4, N512, N128), BF16)
    heads = pltpu.VMEM((N8, N512, N128), F32)
    grad = pltpu.VMEM((2, N512, N128), F32)
    inner = pl.pallas_call(
        attention_kernel,
        out_shape=[act, act, bufs[0]],
        in_specs=[hbm] * 6,
        out_specs=[vmem] * 3,
        scratch_shapes=[act] * 6 + [sem((6,)),
            act, act, pltpu.VMEM((2, N4, N512, N128), BF16), pairs, pairs, pltpu.VMEM((2, N4, N512, N128), BF16),
            pltpu.VMEM((N4, N4, N256, N128), BF16), pltpu.VMEM((N4, N4, N256, N128), BF16), pltpu.VMEM((2, N512, N128), BF16),
            heads, heads, heads, heads, heads,
            grad, grad, grad, act, pltpu.VMEM((3, N512, N512), BF16),
            pltpu.VMEM((2, N16, N128), F32), pltpu.VMEM((N4, N16, N128), F32), pltpu.VMEM((N768, N128), F32), pltpu.VMEM((N4, N16, N128), F32),
            sem((N4,)), sem((N4,)), sem((N4, N4)), sem((N4, N4)), sem, sem, sem((N4,)), sem((N4,)),
            pltpu.VMEM((N4, 2048, N128), F32),
        ] + bufs[1:] + sems,
        compiler_params=pltpu.CompilerParams(collective_id=0, has_side_effects=True, vmem_limit_bytes=58 * 2 ** 20),
        name="attention_step",
    )(x_loc, w_q, w_k, w_v, w_o, dy_loc)
    return pl.pallas_call(
        write_kernel,
        out_shape=[jax.ShapeDtypeStruct((N512, N512), BF16)] * 2 + [jax.ShapeDtypeStruct((N512, N512), F32)] * N4,
        in_specs=[vmem] * 3,
        out_specs=[hbm] * 6,
        scratch_shapes=[sem((N4, 7)), sem((2,))],
        compiler_params=pltpu.CompilerParams(vmem_limit_bytes=N8 * 2 ** 20),
        name="write_results",
    )(*inner)


def solution(mesh):
    def device_step(x_loc, w_q, w_k, w_v, w_o, dy_loc):
        return tuple(attention(x_loc, w_q, w_k, w_v, w_o, dy_loc))

    row_spec = P(("dp", "sp"), None)
    full_spec = P(None, None)
    grad_spec = P("dp", None)
    return jax.shard_map(device_step, mesh=mesh, in_specs=(row_spec, full_spec, full_spec, full_spec, full_spec, row_spec),
                         out_specs=(row_spec, row_spec, grad_spec, grad_spec, grad_spec, grad_spec), check_vma=False)
```
